32 devices in a mesh: pair: 8 (over z, x), aux: 4 (over y, core).
Axes of the slice: x: 2, y: 2, z: 4, core: 2. Of those that a mesh axis runs over, the one named last changes fastest.
Arguments:
- panels: bfloat16 [16, 120, 9216], P('pair', None, 'aux'), may hold values from -1.5 to 1.5
- amplitudes: bfloat16 [16, 2, 120, 120], P('pair'), may hold values from -0.5 to 0.5
- drive: float32 [16, 2, 14400], P('pair', None, 'aux'), may hold values from -6 to 6
- pno_energy: float32 [16, 120], P('pair'), may hold values from 1 to 3
- occ_energy: float32 [32], replicated, may hold values from -2 to -0.5
- frequency: float32 [1], replicated, may hold values from 0.2 to 2
- pair_lmo: int32 [16, 2], replicated, may hold values from 0 to 31
- neighbours: int32 [16, 8], P('pair'), may hold values from 0 to 15
- pno_ranks: int32 [16], P('pair'), may hold values from 60 to 120
- fock_off: float32 [32, 32], replicated, may hold values from -1.8 to 1.8
Outputs:
- residual: float32 [16, 2, 14400], P('pair', None, 'aux')
The draws below stay inside these ranges and needn't reach their ends.
Inputs may be any that keep to these rules, and one draw needn't show every extreme that they name: `neighbours`: neighbour pairs; a pair may be listed more than once and may list itself. `pno_ranks`: rows of a pair's panel from its rank on are padding.
All inputs are finite; a program needn't handle non-finite values.
Results may differ from the reference program's by a relative error of at most 0.0033.
Values may be sent and summed in bfloat16 or wider, within the bound.
No kernel may reach another device: no remote copies, remote signals or barrier semaphores. Data moves between devices by JAX's collectives and lax.ppermute only.
A program may use at most 128 MiB of HBM per device.

```python
import jax
import jax.numpy as jnp
from jax import lax

R = 120
AUX_DEV = 2304
AUX = 9216
PAIRS = 16
NBR = 8
NLMO = 32
RR = 14400
N_AUX = 4


def plant(values, rng, least, high):
    longest = values.shape.index(max(values.shape))
    spots = []
    for shift in (0, 1):
        where = [jax.random.randint(jax.random.fold_in(rng, axis), (), 0, length) for axis, length in enumerate(values.shape)]
        where[longest] = (where[longest] + shift) % values.shape[longest]
        spots.append(tuple(where))
    return values.at[spots[0]].set(least).at[spots[1]].set(high)


def levels(own_key, shape, pieces, least, largest):
    def one(axis_at, shards_of):
        draws = jax.random.uniform(jax.random.fold_in(jax.random.fold_in(own_key, 6), axis_at), (shards_of,), jnp.float32, least / len(pieces), largest / len(pieces))
        return jnp.repeat(jnp.exp(draws), shape[axis_at] // shards_of).reshape((-1,) + (1,) * (len(shape) - axis_at - 1))

    loudness = one(*pieces[0])
    for cut in pieces[1:]:
        loudness = loudness * one(*cut)
    return loudness


def bell_draw(rng, dims, width, reach, split=(), kind=jnp.bfloat16):
    entries = jax.random.normal(rng, dims, jnp.float32) * width
    if len(split) > 0:
        entries = levels(rng, dims, split, -0.22, 0.18) * entries
    return jnp.clip(entries, min=-reach, max=reach).astype(kind)


def setup_inputs(seed: int = 0) -> dict:
    splits = jax.random.split(jax.random.key(seed), 11)
    return {
        "panels": bell_draw(splits[0], (PAIRS, R, AUX), (AUX ** -0.25), 1.5, ((0, 8), (2, 4))),
        "amplitudes": bell_draw(splits[1], (PAIRS, 2, R, R), R ** -0.5, 0.5, ((0, 8),)),
        "drive": bell_draw(splits[2], (PAIRS, 2, RR), 1.0, 6.0, ((0, 8), (2, 4)), jnp.float32),
        "pno_energy": jnp.clip(1.0 + 2.0 * jax.random.uniform(splits[3], (PAIRS, R), jnp.float32) ** levels(splits[3], (PAIRS, R), ((0, 8),), -0.2, 0.2), 1.0, 3.0),
        "occ_energy": jnp.clip(jax.random.uniform(splits[4], (NLMO,), jnp.float32, -2.0, -0.5), -2.0, -0.5),
        "frequency": jnp.clip(jax.random.uniform(splits[5], (1,), jnp.float32, 0.2, 2.0), 0.2, 2.0),
        "pair_lmo": plant(jax.random.randint(splits[6], (PAIRS, 2), 0, NLMO), jax.random.fold_in(splits[6], 1), 0, NLMO - 1).astype(jnp.int32),
        "neighbours": plant(jax.random.randint(splits[7], (PAIRS, NBR), 0, PAIRS), jax.random.fold_in(splits[7], 1), 0, PAIRS - 1).astype(jnp.int32),
        "pno_ranks": plant(jax.random.randint(splits[8], (PAIRS,), R // 2, R + 1), jax.random.fold_in(splits[8], 1), R // 2, R).astype(jnp.int32),
        "fock_off": bell_draw(splits[9], (NLMO, NLMO), 0.3, 1.8, (), jnp.float32),
    }


def reference(panels, amplitudes, drive, pno_energy, occ_energy, frequency, pair_lmo, neighbours, pno_ranks, fock_off):
    rows_index = jnp.arange(R, dtype=jnp.int32)
    keep_rows = rows_index[None, :] < pno_ranks[:, None]
    masked = jnp.where(keep_rows[:, :, None], panels, jnp.zeros_like(panels))
    near_lmo = pair_lmo[neighbours]
    values = fock_off[pair_lmo[:, 0][:, None], near_lmo[:, :, 0]] + fock_off[pair_lmo[:, 1][:, None], near_lmo[:, :, 1]]
    onehot = (neighbours[:, :, None] == jnp.arange(PAIRS, dtype=jnp.int32)[None, None, :]).astype(jnp.float32)
    weights = jnp.sum(values[:, :, None] * onehot, axis=1).astype(jnp.bfloat16)
    weights_wide = weights.astype(jnp.float32)
    matrices = jnp.transpose(amplitudes, (0, 2, 1, 3)).reshape(PAIRS, R, 2 * R).astype(jnp.float32)

    def block_step(running_sum, block_index):
        start_col = (block_index * AUX_DEV).astype(jnp.int32)
        slab = lax.dynamic_slice_in_dim(masked, start_col, AUX_DEV, 2).astype(jnp.float32)
        projected = jnp.einsum('nra,nrc->nac', slab, matrices, precision=lax.Precision.HIGHEST).astype(jnp.bfloat16)
        projected = lax.optimization_barrier(projected).astype(jnp.float32)
        collected = jnp.einsum('pn,nac->pac', weights_wide, projected, precision=lax.Precision.HIGHEST).astype(jnp.bfloat16)
        collected = lax.optimization_barrier(collected).astype(jnp.float32)
        running_sum = running_sum + jnp.einsum('pra,pac->prc', slab, collected, precision=lax.Precision.HIGHEST)
        return running_sum, None

    start_sum = jnp.zeros((PAIRS, R, 2 * R), jnp.float32)
    coupled, unused_out = lax.scan(block_step, start_sum, jnp.arange(N_AUX, dtype=jnp.int32))
    coupled = jnp.transpose(coupled.reshape(PAIRS, R, 2, R), (0, 2, 1, 3))
    occ_pair = occ_energy[pair_lmo[:, 0]] + occ_energy[pair_lmo[:, 1]]
    shift = pno_energy[:, :, None] + pno_energy[:, None, :] - occ_pair[:, None, None]
    signs = jnp.array([1.0, -1.0], jnp.float32)
    factor = shift[:, None, :, :] - signs[None, :, None, None] * frequency[0]
    diagonal_term = factor * amplitudes.astype(jnp.float32)
    return drive + diagonal_term.reshape(PAIRS, 2, R * R) + coupled.reshape(PAIRS, 2, R * R)
```

```python
import functools

import jax
import jax.numpy as jnp
from jax import lax
from jax.experimental import pallas as pl
from jax.experimental.pallas import tpu as pltpu
from jax.sharding import PartitionSpec as P

LANES = 128
BF = jnp.bfloat16
F32 = jnp.float32


def round_up(value, unit):
    return -(-value // unit) * unit


def pair_weights(pair_lmo, neighbours, fock_off, first_pair):
    local_pairs = neighbours.shape[0]
    total_pairs = pair_lmo.shape[0]
    lmo_count = fock_off.shape[0]
    lmo_ids = jnp.arange(lmo_count, dtype=jnp.int32)
    own_lmo = lax.dynamic_slice_in_dim(pair_lmo, first_pair, local_pairs, 0)
    own_table = (own_lmo[:, :, None] == lmo_ids[None, None, :]).astype(F32)
    lmo_table = (pair_lmo[:, :, None] == lmo_ids[None, None, :]).astype(F32)
    pair_ids = jnp.arange(total_pairs, dtype=jnp.int32)
    onehot = (neighbours[:, :, None] == pair_ids[None, None, :]).astype(F32)
    fock_rows = jnp.einsum("psl,lm->psm", own_table, fock_off, precision=lax.Precision.HIGHEST)
    near_table = jnp.einsum("pkn,nsl->pksl", onehot, lmo_table)
    values = jnp.sum(fock_rows[:, None, :, :] * near_table, axis=(2, 3))
    weights = jnp.sum(values[:, :, None] * onehot, axis=1).astype(BF)
    return (weights, own_table)


def couple_kernel(blocks, aux_ref, w_ref, x_ref, a_ref, out_ref, proj_ref):
    total, width, depth = x_ref.shape
    freqs = a_ref.shape[1]
    lanes = a_ref.shape[3]
    local = out_ref.shape[3]
    rows = depth // blocks
    my_core = aux_ref[0] % 2

    def project(n, carry):
        x = x_ref[n]
        for s in range(freqs):
            proj_ref[n, :, s * lanes : (s + 1) * lanes] = jnp.dot(
                x, a_ref[n, s], preferred_element_type=F32
            )
        return carry

    lax.fori_loop(0, total, project, 0)

    def close(p, carry):
        acc = w_ref[p, 0] * proj_ref[0]
        for n in range(1, total):
            acc = acc + w_ref[p, n] * proj_ref[n]
        got = lax.dot_general(
            x_ref[p], acc.astype(BF), (((0,), (0,)), ((), ())), preferred_element_type=F32
        )
        for h in range(blocks):
            side = (my_core + h) % 2 if blocks > 1 else 0
            for s in range(freqs):
                out_ref[side, p // local, h // 2, p % local, s] = got[
                    h * rows : (h + 1) * rows, s * lanes : (s + 1) * lanes
                ].astype(out_ref.dtype)
        return carry

    lax.fori_loop(0, total, close, 0)


def body(sizes, panels, amplitudes, drive, pno_energy, occ_energy, frequency, pair_lmo,
         neighbours, pno_ranks, fock_off):
    n_pair, n_aux = sizes
    local, rank, width = panels.shape
    freqs = amplitudes.shape[1]
    total = pair_lmo.shape[0]
    even = rank % n_aux == 0 and n_aux % 2 == 0
    blocks = n_aux if even else 1
    rows = rank // blocks
    rows_pad = round_up(rows, 16)
    depth = round_up(blocks * rows_pad, LANES)
    rows_pad = depth // blocks
    part = width // n_pair
    me_pair = lax.axis_index("pair")
    me_aux = lax.axis_index("aux")

    weights, own_table = pair_weights(pair_lmo, neighbours, fock_off, me_pair * local)

    keep = jnp.arange(rank, dtype=jnp.int32)[None, :] < pno_ranks[:, None]
    masked = jnp.where(keep[:, :, None], panels, jnp.zeros_like(panels))
    spread = jnp.pad(
        masked.reshape(local, blocks, rows, width), ((0, 0), (0, 0), (0, rows_pad - rows), (0, 0))
    ).reshape(local, depth, n_pair, part)
    spread = jnp.transpose(spread, (2, 0, 3, 1)).reshape(n_pair, local * part, depth)
    amp = jnp.pad(
        amplitudes.reshape(local, freqs, blocks, rows, rank),
        ((0, 0), (0, 0), (0, 0), (0, rows_pad - rows), (0, LANES - rank)),
    ).reshape(n_aux, -1, LANES)
    amp_rows = amp.shape[1]
    share = lax.dynamic_index_in_dim(amp, me_aux, 0, keepdims=False)
    tail = jnp.pad(weights, ((0, 16 - local), (0, LANES - total)))
    extra = jnp.concatenate([share, tail], axis=0)
    sent = jnp.concatenate(
        [spread, jnp.broadcast_to(extra[None], (n_pair,) + extra.shape)], axis=1
    )
    got = lax.all_to_all(sent, "pair", 0, 0, tiled=True)
    xt = got[:, : local * part].reshape(total, part, depth)
    w_all = got[:, local * part + amp_rows :][:, :local, :total].reshape(total, total).astype(F32)
    mats = got[:, local * part : local * part + amp_rows][None]
    step = n_aux // 2
    while step >= 1:
        other = lax.ppermute(mats, "aux", [(i, i ^ step) for i in range(n_aux)])
        mats = jnp.concatenate([mats, other], axis=0)
        step //= 2
    order = []
    for member in range(n_aux):
        j, bit, step = 0, 1, n_aux // 2
        slot = jnp.int32(0)
        while step >= 1:
            slot = slot + bit * (((me_aux ^ member) & step) > 0).astype(jnp.int32)
            bit, step = bit * 2, step // 2
        order.append(lax.dynamic_index_in_dim(mats, slot, 0, keepdims=False))
    mats = jnp.stack(order, axis=1).reshape(total, freqs, depth, LANES)

    out_dims = (2 if even else 1, n_pair, max(blocks // 2, 1), local, freqs, rows_pad, LANES)
    vmem = pl.BlockSpec(memory_space=pltpu.VMEM)
    smem = pl.BlockSpec(memory_space=pltpu.SMEM)
    flops = 4 * total * part * depth * freqs * LANES
    coupled = pl.pallas_call(
        functools.partial(couple_kernel, blocks),
        out_shape=jax.ShapeDtypeStruct(out_dims, BF if even else F32),
        in_specs=[smem, smem, vmem, vmem],
        out_specs=vmem,
        scratch_shapes=[pltpu.VMEM((total, part, freqs * LANES), F32)],
        compiler_params=pltpu.CompilerParams(vmem_limit_bytes=40 * 2**20),
        cost_estimate=pl.CostEstimate(flops=flops, bytes_accessed=4 * 2**20, transcendentals=0),
    )(me_aux.reshape(1), w_all, xt, mats)

    if even:
        other = lax.ppermute(coupled[1], "aux", [(i, i ^ 1) for i in range(n_aux)])
        mine = (coupled[0].astype(F32) + other.astype(F32)).astype(BF)
        mine = mine.reshape((n_pair * (n_aux // 2),) + out_dims[3:])
        groups = [
            [g * n_aux + 2 * h + c for g in range(n_pair) for h in range(n_aux // 2)]
            for c in range(2)
        ]
        parts = lax.all_to_all(
            mine, ("pair", "aux"), 0, 0, axis_index_groups=groups, tiled=True
        )
        coupled_share = jnp.sum(parts.astype(F32), axis=0)[:, :, :rows, :rank].reshape(
            local, freqs, rows * rank
        )
    else:
        flat = coupled.reshape(total, freqs, depth, LANES)[:, :, :rank, :rank]
        flat = flat.reshape(total, freqs, rank * rank)
        share_aux = lax.psum_scatter(flat, "aux", scatter_dimension=2, tiled=True)
        coupled_share = lax.psum_scatter(share_aux, "pair", scatter_dimension=0, tiled=True)

    share_width = drive.shape[2]
    start = me_aux * share_width
    occ_pair = jnp.sum(own_table * occ_energy[None, None, :], axis=(1, 2))
    shift = pno_energy[:, :, None] + pno_energy[:, None, :] - occ_pair[:, None, None]
    signs = jnp.array([1.0, -1.0], F32)
    if even:
        energy_rows = lax.dynamic_slice_in_dim(pno_energy, me_aux * rows, rows, 1)
        shift = energy_rows[:, :, None] + pno_energy[:, None, :] - occ_pair[:, None, None]
        factor = shift[:, None] - signs[None, :, None, None] * frequency[0]
        amp_rows_own = lax.dynamic_slice_in_dim(amplitudes, me_aux * rows, rows, 2)
        diagonal = (factor * amp_rows_own.astype(F32)).reshape(local, freqs, share_width)
    else:
        factor = shift[:, None] - signs[None, :, None, None] * frequency[0]
        diagonal = (factor * amplitudes.astype(F32)).reshape(local, freqs, rank * rank)
        diagonal = lax.dynamic_slice_in_dim(diagonal, start, share_width, 2)
    return drive + diagonal + coupled_share


def solution(mesh):
    placed = (
        P("pair", None, "aux"),
        P("pair", None, None, None),
        P("pair", None, "aux"),
        P("pair", None),
        P(),
        P(),
        P(),
        P("pair", None),
        P("pair"),
        P(),
    )
    sizes = (mesh.shape["pair"], mesh.shape["aux"])
    return jax.shard_map(
        functools.partial(body, sizes),
        mesh=mesh,
        in_specs=placed,
        out_specs=P("pair", None, "aux"),
        check_vma=False,
    )
```

```python
import functools

import jax
import jax.numpy as jnp
from jax import lax
from jax.experimental import pallas as pl
from jax.experimental.pallas import tpu as pltpu
from jax.sharding import PartitionSpec as P

LANES = 128
BF = jnp.bfloat16
F32 = jnp.float32


def round_up(value, unit):
    return -(-value // unit) * unit


def flip(count, bits):
    return [(i, i ^ bits) for i in range(count)]


def prep_kernel(n_pair, blocks, rows, where, lmo, near, ranks, fock, panels, amps, *outs):
    chunks, share_ref, turned = outs[:n_pair], outs[n_pair], outs[n_pair + 1]
    local, rank, width = panels.shape
    depth = turned.shape[2]
    rows_pad = depth // blocks
    part = width // n_pair
    me = where[0]
    freq = where[1]
    slots = near.shape[1]

    def spread_rows(x, lanes):
        pieces = []
        for h in range(blocks):
            pieces.append(x[h * rows : (h + 1) * rows])
            if rows_pad > rows:
                pieces.append(jnp.zeros((rows_pad - rows, lanes), x.dtype))
        return jnp.concatenate(pieces, axis=0) if len(pieces) > 1 else pieces[0]

    tile = 256 if width % 256 == 0 else LANES
    for lp in range(local):
        keep = lax.broadcasted_iota(jnp.int32, (rank, tile), 0) < ranks[lp]
        for t in range(width // tile):
            x = panels[lp, :, t * tile : (t + 1) * tile].astype(F32)
            x = spread_rows(jnp.where(keep, x, 0.0), tile)
            turned[lp, t * tile : (t + 1) * tile, :] = x.T.astype(BF)
    for k in range(n_pair):
        start = pl.multiple_of((me ^ k) * part, 16)
        for lp in range(local):
            chunks[k][lp] = turned[lp, pl.ds(start, part), :]

    share_rows = share_ref.shape[0]
    freqs = amps.shape[1] * depth * local // (share_rows - 16)
    take = amps.shape[1] // freqs
    for lp in range(local):
        for s in range(take):
            a = amps[lp, freq * take + s].astype(F32)
            a = spread_rows(a, rank)
            a = jnp.concatenate([a, jnp.zeros((depth, LANES - rank), F32)], axis=1)
            first = (lp * take + s) * depth
            share_ref[first : first + depth, :] = a.astype(BF)

    row = lax.broadcasted_iota(jnp.int32, (16, LANES), 0)
    lane = lax.broadcasted_iota(jnp.int32, (16, LANES), 1)
    tail = jnp.zeros((16, LANES), F32)
    for lp in range(local):
        left, right = lmo[me * local + lp, 0], lmo[me * local + lp, 1]
        ids = [near[lp, k] for k in range(slots)]
        values = [fock[left, lmo[i, 0]] + fock[right, lmo[i, 1]] for i in ids]
        for k in range(slots):
            total = jnp.float32(0.0)
            fresh = jnp.float32(1.0)
            for j in range(slots):
                same = (ids[j] == ids[k]).astype(F32) if j != k else jnp.float32(1.0)
                total = total + same * values[j]
                if j < k:
                    fresh = fresh * (1.0 - same)
            here = lane == lp * slots + k
            tail = jnp.where(here & (row == 0), ids[k].astype(F32), tail)
            tail = jnp.where(here & (row == 1), total * fresh, tail)
    share_ref[share_rows - 16 :, :] = tail.astype(BF)


def couple_kernel(n_pair, blocks, where, ids_ref, w_ref, *refs):
    panels, mats, out_ref, proj, mixed = refs[:n_pair], *refs[n_pair:]
    local, part, depth = panels[0].shape
    freqs = proj.shape[2] // LANES
    rows = depth // blocks
    slots = ids_ref.shape[2]
    me, my_core = where[0], where[1]
    sides = mats.shape[0]
    take = freqs // sides

    for k in range(n_pair):
        for lp in range(local):
            for s in range(freqs):
                side, inner = s // take, s % take
                slot = my_core ^ side if sides == 2 else 0
                first = (lp * take + inner) * depth
                proj[k * local + lp, :, s * LANES : (s + 1) * LANES] = jnp.dot(
                    panels[k][lp],
                    mats[slot, k, first : first + depth, :],
                    preferred_element_type=F32,
                )

    tile = 32 if part % 32 == 0 else 16
    for k in range(n_pair):
        for lp in range(local):
            source = []
            for j in range(slots):
                i = ids_ref[k, lp, j]
                source.append(((i // local) ^ me) * local + i % local)
            scale = [w_ref[k, lp, j] for j in range(slots)]
            for t in range(part // tile):
                span = slice(t * tile, (t + 1) * tile)
                acc = scale[0] * proj[source[0], span, :]
                for j in range(1, slots):
                    acc = acc + scale[j] * proj[source[j], span, :]
                mixed[span, :] = acc.astype(BF)
            got = lax.dot_general(
                panels[k][lp], mixed[...], (((0,), (0,)), ((), ())), preferred_element_type=F32
            )
            for h in range(blocks):
                side = my_core ^ (h % 2) if blocks > 1 else 0
                for s in range(freqs):
                    out_ref[side, me ^ k, h // 2, lp, s] = got[
                        h * rows : (h + 1) * rows, s * LANES : (s + 1) * LANES
                    ].astype(out_ref.dtype)


def body(sizes, panels, amplitudes, drive, pno_energy, occ_energy, frequency, pair_lmo,
         neighbours, pno_ranks, fock_off):
    n_pair, n_aux = sizes
    local, rank, width = panels.shape
    freqs = amplitudes.shape[1]
    total = pair_lmo.shape[0]
    slots = neighbours.shape[1]
    even = rank % n_aux == 0 and n_aux % 2 == 0
    blocks = n_aux if even else 1
    rows = rank // blocks
    rows_pad = round_up(rows, 16)
    depth = round_up(blocks * rows_pad, LANES)
    rows_pad = depth // blocks
    part = width // n_pair
    me_pair = lax.axis_index("pair")
    me_aux = lax.axis_index("aux")
    sides = 2 if n_aux % 2 == 0 and freqs % 2 == 0 else 1
    my_core = me_aux % 2 if sides == 2 else jnp.int32(0)
    where = jnp.stack([me_pair, my_core]).astype(jnp.int32)
    vmem = pl.BlockSpec(memory_space=pltpu.VMEM)
    smem = pl.BlockSpec(memory_space=pltpu.SMEM)

    share_rows = local * (freqs // sides) * depth + 16
    outs = pl.pallas_call(
        functools.partial(prep_kernel, n_pair, blocks, rows),
        out_shape=[jax.ShapeDtypeStruct((local, part, depth), BF)] * n_pair
        + [jax.ShapeDtypeStruct((share_rows, LANES), BF)],
        in_specs=[smem] * 5 + [vmem] * 2,
        out_specs=[vmem] * (n_pair + 1),
        scratch_shapes=[pltpu.VMEM((local, width, depth), BF)],
        compiler_params=pltpu.CompilerParams(vmem_limit_bytes=24 * 2**20),
        cost_estimate=pl.CostEstimate(flops=0, bytes_accessed=4 * 2**20, transcendentals=0),
    )(where, pair_lmo, neighbours, pno_ranks, fock_off, panels, amplitudes)
    chunks, share = outs[:n_pair], outs[n_pair]

    steps = [1 << b for b in reversed(range(n_pair.bit_length() - 1))]
    if len(steps) > 2:
        steps = [steps[0]] + steps[:0:-1]
    held = {0: share}
    for step in steps:
        keys = sorted(held)
        stacked = jnp.concatenate([held[key][None] for key in keys], axis=0)
        other = lax.ppermute(stacked, "pair", flip(n_pair, step))
        for slot, key in enumerate(keys):
            held[key ^ step] = other[slot]
    mats = jnp.concatenate([held[key][None] for key in range(n_pair)], axis=0)[None]
    received = [chunks[0]] + [None] * (n_pair - 1)
    for k in reversed(range(1, n_pair)):
        received[k] = lax.ppermute(chunks[k], "pair", flip(n_pair, k))
    tail = mats[0, :, share_rows - 16 :]
    ids = tail[:, 0, : local * slots].reshape(n_pair, local, slots).astype(jnp.int32)
    scale = tail[:, 1, : local * slots].reshape(n_pair, local, slots).astype(F32)
    if sides == 2:
        mats = jnp.concatenate([mats, lax.ppermute(mats, "aux", flip(n_aux, 1))], axis=0)

    out_dims = (2 if even else 1, n_pair, max(blocks // 2, 1), local, freqs, rows_pad, LANES)
    flops = 4 * total * part * depth * freqs * LANES
    coupled = pl.pallas_call(
        functools.partial(couple_kernel, n_pair, blocks),
        out_shape=jax.ShapeDtypeStruct(out_dims, BF if even else F32),
        in_specs=[smem] * 3 + [vmem] * (n_pair + 1),
        out_specs=vmem,
        scratch_shapes=[
            pltpu.VMEM((total, part, freqs * LANES), F32),
            pltpu.VMEM((part, freqs * LANES), BF),
        ],
        compiler_params=pltpu.CompilerParams(vmem_limit_bytes=40 * 2**20),
        cost_estimate=pl.CostEstimate(flops=flops, bytes_accessed=4 * 2**20, transcendentals=0),
    )(where, ids, scale, *received, mats)

    if even:
        other = lax.ppermute(coupled[1], "aux", flip(n_aux, 1))
        mine = (coupled[0].astype(F32) + other.astype(F32)).astype(BF)
        mine = mine.reshape((n_pair * (n_aux // 2),) + out_dims[3:])
        groups = [
            [g * n_aux + 2 * h + c for g in range(n_pair) for h in range(n_aux // 2)]
            for c in range(2)
        ]
        parts = lax.all_to_all(
            mine, ("pair", "aux"), 0, 0, axis_index_groups=groups, tiled=True
        )
        coupled_share = jnp.sum(parts.astype(F32), axis=0)[:, :, :rows, :rank].reshape(
            local, freqs, rows * rank
        )
    else:
        flat = coupled.reshape(total, freqs, depth, LANES)[:, :, :rank, :rank]
        flat = flat.reshape(total, freqs, rank * rank)
        share_aux = lax.psum_scatter(flat, "aux", scatter_dimension=2, tiled=True)
        coupled_share = lax.psum_scatter(share_aux, "pair", scatter_dimension=0, tiled=True)

    share_width = drive.shape[2]
    start = me_aux * share_width
    lmo_ids = jnp.arange(occ_energy.shape[0], dtype=jnp.int32)
    own_lmo = lax.dynamic_slice_in_dim(pair_lmo, me_pair * local, local, 0)
    own_table = (own_lmo[:, :, None] == lmo_ids[None, None, :]).astype(F32)
    occ_pair = jnp.sum(own_table * occ_energy[None, None, :], axis=(1, 2))
    signs = jnp.array([1.0, -1.0], F32)
    if even:
        energy_rows = lax.dynamic_slice_in_dim(pno_energy, me_aux * rows, rows, 1)
        shift = energy_rows[:, :, None] + pno_energy[:, None, :] - occ_pair[:, None, None]
        factor = shift[:, None] - signs[None, :, None, None] * frequency[0]
        amp_rows_own = lax.dynamic_slice_in_dim(amplitudes, me_aux * rows, rows, 2)
        diagonal = (factor * amp_rows_own.astype(F32)).reshape(local, freqs, share_width)
    else:
        shift = pno_energy[:, :, None] + pno_energy[:, None, :] - occ_pair[:, None, None]
        factor = shift[:, None] - signs[None, :, None, None] * frequency[0]
        diagonal = (factor * amplitudes.astype(F32)).reshape(local, freqs, rank * rank)
        diagonal = lax.dynamic_slice_in_dim(diagonal, start, share_width, 2)
    return drive + diagonal + coupled_share


def solution(mesh):
    placed = (
        P("pair", None, "aux"),
        P("pair", None, None, None),
        P("pair", None, "aux"),
        P("pair", None),
        P(),
        P(),
        P(),
        P("pair", None),
        P("pair"),
        P(),
    )
    sizes = (mesh.shape["pair"], mesh.shape["aux"])
    return jax.shard_map(
        functools.partial(body, sizes),
        mesh=mesh,
        in_specs=placed,
        out_specs=P("pair", None, "aux"),
        check_vma=False,
    )
```

```python
import functools

import jax
import jax.numpy as jnp
from jax import lax
from jax.experimental import pallas as pl
from jax.experimental.pallas import tpu as pltpu
from jax.sharding import PartitionSpec as P


LANES = 128
BF = jnp.bfloat16
F32 = jnp.float32


def round_up(value, unit):
    return -(-value // unit) * unit


def flip(count, bits):
    return [(i, i ^ bits) for i in range(count)]


def prep_kernel(n_pair, blocks, rows, sides, *refs):
    inputs, chunks, share_ref = refs[:6], refs[6 : 6 + n_pair], refs[6 + n_pair]
    buffers, (turned, sems) = refs[7 + n_pair : 13 + n_pair], refs[13 + n_pair :]
    copies = [
        pltpu.make_async_copy(src, dst, sems.at[i])
        for i, (src, dst) in enumerate(zip(inputs, buffers))
    ]
    for copy in copies:
        copy.start()
    panels, amps, lmo, near, ranks, fock = buffers
    local, rank, width = panels.shape
    depth = turned.shape[2]
    rows_pad = depth // blocks
    part = width // n_pair
    me = lax.axis_index("pair")
    freq = lax.axis_index("aux") % 2 if sides == 2 else 0
    slots = near.shape[1]
    for copy in copies:
        copy.wait()

    def spread_rows(x, lanes):
        pieces = []
        for h in range(blocks):
            pieces.append(x[h * rows : (h + 1) * rows])
            if rows_pad > rows:
                pieces.append(jnp.zeros((rows_pad - rows, lanes), x.dtype))
        return jnp.concatenate(pieces, axis=0) if len(pieces) > 1 else pieces[0]

    tile = 256 if width % 256 == 0 else LANES
    for lp in range(local):
        keep = lax.broadcasted_iota(jnp.int32, (rank, tile), 0) < ranks[lp]
        for t in range(width // tile):
            x = panels[lp, :, t * tile : (t + 1) * tile].astype(F32)
            x = spread_rows(jnp.where(keep, x, 0.0), tile)
            turned[lp, t * tile : (t + 1) * tile, :] = x.T.astype(BF)
    for k in range(n_pair):
        start = pl.multiple_of((me ^ k) * part, 16)
        for lp in range(local):
            chunks[k][lp] = turned[lp, pl.ds(start, part), :]

    share_rows = share_ref.shape[0]
    freqs = amps.shape[1] * depth * local // (share_rows - 16)
    take = amps.shape[1] // freqs
    for lp in range(local):
        for s in range(take):
            a = amps[lp, freq * take + s].astype(F32)
            a = spread_rows(a, rank)
            a = jnp.concatenate([a, jnp.zeros((depth, LANES - rank), F32)], axis=1)
            first = (lp * take + s) * depth
            share_ref[first : first + depth, :] = a.astype(BF)

    row = lax.broadcasted_iota(jnp.int32, (16, LANES), 0)
    lane = lax.broadcasted_iota(jnp.int32, (16, LANES), 1)
    tail = jnp.zeros((16, LANES), F32)
    for lp in range(local):
        left, right = lmo[0, me * local + lp], lmo[1, me * local + lp]
        ids = [near[lp, k] for k in range(slots)]
        values = [fock[left, lmo[0, i]] + fock[right, lmo[1, i]] for i in ids]
        for k in range(slots):
            total = jnp.float32(0.0)
            fresh = jnp.float32(1.0)
            for j in range(slots):
                same = (ids[j] == ids[k]).astype(F32) if j != k else jnp.float32(1.0)
                total = total + same * values[j]
                if j < k:
                    fresh = fresh * (1.0 - same)
            here = lane == lp * slots + k
            tail = jnp.where(here & (row == 0), ids[k].astype(F32), tail)
            tail = jnp.where(here & (row == 1), total * fresh, tail)
    share_ref[share_rows - 16 :, :] = tail.astype(BF)


def couple_kernel(n_pair, blocks, sides, where, ids_ref, w_ref, *refs):
    half = n_pair // 2
    panels, mats = refs[:n_pair], refs[n_pair : n_pair + half * sides]
    out_ref, proj, mixed = refs[n_pair + half * sides :]
    local, part, depth = panels[0].shape
    freqs = proj.shape[2] // LANES
    rows = depth // blocks
    slots = ids_ref.shape[2]
    me, my_core = where[0], where[1]
    take = freqs // sides

    for k in range(n_pair):
        for lp in range(local):
            for s in range(freqs):
                slot, inner = s // take, s % take
                first = (lp * take + inner) * depth
                mat = mats[slot * half + k % half][k // half, first : first + depth, :]
                proj[k * local + lp, :, s * LANES : (s + 1) * LANES] = jnp.dot(
                    panels[k][lp], mat, preferred_element_type=F32
                )

    tile = 32 if part % 32 == 0 else 16
    for k in range(n_pair):
        for lp in range(local):
            source = []
            for j in range(slots):
                i = ids_ref[k, lp, j]
                source.append(((i // local) ^ me) * local + i % local)
            scale = [w_ref[k, lp, j] for j in range(slots)]
            for t in range(part // tile):
                span = slice(t * tile, (t + 1) * tile)
                acc = scale[0] * proj[source[0], span, :]
                for j in range(1, slots):
                    acc = acc + scale[j] * proj[source[j], span, :]
                mixed[span, :] = acc.astype(BF)
            got = lax.dot_general(
                panels[k][lp], mixed[...], (((0,), (0,)), ((), ())), preferred_element_type=F32
            )
            for h in range(blocks):
                side = my_core ^ (h % 2) if blocks > 1 else 0
                for s in range(freqs):
                    freq = (s // take ^ my_core) * take + s % take if sides == 2 else s
                    out_ref[side, me ^ k, h // 2, lp, freq] = got[
                        h * rows : (h + 1) * rows, s * LANES : (s + 1) * LANES
                    ].astype(out_ref.dtype)


def body(sizes, panels, amplitudes, drive, pno_energy, occ_energy, frequency, pair_lmo,
         neighbours, pno_ranks, fock_off):
    n_pair, n_aux = sizes
    local, rank, width = panels.shape
    freqs = amplitudes.shape[1]
    total = pair_lmo.shape[0]
    slots = neighbours.shape[1]
    even = rank % n_aux == 0 and n_aux % 2 == 0
    blocks = n_aux if even else 1
    rows = rank // blocks
    rows_pad = round_up(rows, 16)
    depth = round_up(blocks * rows_pad, LANES)
    rows_pad = depth // blocks
    part = width // n_pair
    me_pair = lax.axis_index("pair")
    me_aux = lax.axis_index("aux")
    sides = 2 if n_aux % 2 == 0 and freqs % 2 == 0 else 1
    my_core = me_aux % 2 if sides == 2 else jnp.int32(0)
    where = jnp.stack([me_pair, my_core]).astype(jnp.int32)
    vmem = pl.BlockSpec(memory_space=pltpu.VMEM)
    smem = pl.BlockSpec(memory_space=pltpu.SMEM)

    share_rows = local * (freqs // sides) * depth + 16
    given = (panels, amplitudes, pair_lmo.T, neighbours, pno_ranks, fock_off)
    spaces = [pltpu.VMEM] * 2 + [pltpu.SMEM] * 4
    outs = pl.pallas_call(
        functools.partial(prep_kernel, n_pair, blocks, rows, sides),
        out_shape=[jax.ShapeDtypeStruct((local, part, depth), BF)] * n_pair
        + [jax.ShapeDtypeStruct((share_rows, LANES), BF)],
        in_specs=[pl.BlockSpec(memory_space=pltpu.HBM)] * 6,
        out_specs=[vmem] * (n_pair + 1),
        scratch_shapes=[space(a.shape, a.dtype) for space, a in zip(spaces, given)]
        + [pltpu.VMEM((local, width, depth), BF), pltpu.SemaphoreType.DMA((6,))],
        cost_estimate=pl.CostEstimate(flops=0, bytes_accessed=4 * 2**20, transcendentals=0),
    )(*given)
    chunks, share = outs[:n_pair], outs[n_pair]

    far = n_pair // 2
    other = lax.ppermute(share, "pair", flip(n_pair, far))
    pieces = [jnp.concatenate([share[None], other[None]], axis=0)] + [None] * (far - 1)
    received = [chunks[0]] + [None] * (n_pair - 1)
    for k in range(1, n_pair):
        if k < far:
            pieces[k] = lax.ppermute(pieces[0], "pair", flip(n_pair, k))
        received[k] = lax.ppermute(chunks[k], "pair", flip(n_pair, k))
    tail = jnp.stack([piece[:, share_rows - 16 :] for piece in pieces], axis=1)
    tail = tail.reshape(n_pair, 16, LANES)
    ids = tail[:, 0, : local * slots].reshape(n_pair, local, slots).astype(jnp.int32)
    scale = tail[:, 1, : local * slots].reshape(n_pair, local, slots).astype(F32)
    if sides == 2:
        for k in range(far):
            pieces.append(lax.ppermute(pieces[k], "aux", flip(n_aux, 1)))

    out_dims = (2 if even else 1, n_pair, max(blocks // 2, 1), local, freqs, rows_pad, LANES)
    flops = 4 * total * part * depth * freqs * LANES
    coupled = pl.pallas_call(
        functools.partial(couple_kernel, n_pair, blocks, sides),
        out_shape=jax.ShapeDtypeStruct(out_dims, BF if even else F32),
        in_specs=[smem] * 3 + [vmem] * (n_pair + far * sides),
        out_specs=vmem,
        scratch_shapes=[
            pltpu.VMEM((total, part, freqs * LANES), F32),
            pltpu.VMEM((part, freqs * LANES), BF),
        ],
        compiler_params=pltpu.CompilerParams(vmem_limit_bytes=40 * 2**20),
        cost_estimate=pl.CostEstimate(flops=flops, bytes_accessed=4 * 2**20, transcendentals=0),
    )(where, ids, scale, *received, *pieces)

    if even:
        other = lax.ppermute(coupled[1], "aux", flip(n_aux, 1))
        mine = (coupled[0].astype(F32) + other.astype(F32)).astype(BF)
        mine = mine.reshape((n_pair * (n_aux // 2),) + out_dims[3:])
        groups = [
            [g * n_aux + 2 * h + c for g in range(n_pair) for h in range(n_aux // 2)]
            for c in range(2)
        ]
        parts = lax.all_to_all(
            mine, ("pair", "aux"), 0, 0, axis_index_groups=groups, tiled=True
        )
        coupled_share = jnp.sum(parts.astype(F32), axis=0)[:, :, :rows, :rank].reshape(
            local, freqs, rows * rank
        )
    else:
        flat = coupled.reshape(total, freqs, depth, LANES)[:, :, :rank, :rank]
        flat = flat.reshape(total, freqs, rank * rank)
        share_aux = lax.psum_scatter(flat, "aux", scatter_dimension=2, tiled=True)
        coupled_share = lax.psum_scatter(share_aux, "pair", scatter_dimension=0, tiled=True)

    share_width = drive.shape[2]
    start = me_aux * share_width
    lmo_ids = jnp.arange(occ_energy.shape[0], dtype=jnp.int32)
    own_lmo = lax.dynamic_slice_in_dim(pair_lmo, me_pair * local, local, 0)
    own_table = (own_lmo[:, :, None] == lmo_ids[None, None, :]).astype(F32)
    occ_pair = jnp.sum(own_table * occ_energy[None, None, :], axis=(1, 2))
    signs = jnp.array([1.0, -1.0], F32)
    if even:
        energy_rows = lax.dynamic_slice_in_dim(pno_energy, me_aux * rows, rows, 1)
        shift = energy_rows[:, :, None] + pno_energy[:, None, :] - occ_pair[:, None, None]
        factor = shift[:, None] - signs[None, :, None, None] * frequency[0]
        amp_rows_own = lax.dynamic_slice_in_dim(amplitudes, me_aux * rows, rows, 2)
        diagonal = (factor * amp_rows_own.astype(F32)).reshape(local, freqs, share_width)
    else:
        shift = pno_energy[:, :, None] + pno_energy[:, None, :] - occ_pair[:, None, None]
        factor = shift[:, None] - signs[None, :, None, None] * frequency[0]
        diagonal = (factor * amplitudes.astype(F32)).reshape(local, freqs, rank * rank)
        diagonal = lax.dynamic_slice_in_dim(diagonal, start, share_width, 2)
    return drive + diagonal + coupled_share


def solution(mesh):
    placed = (
        P("pair", None, "aux"),
        P("pair", None, None, None),
        P("pair", None, "aux"),
        P("pair", None),
        P(),
        P(),
        P(),
        P("pair", None),
        P("pair"),
        P(),
    )
    sizes = (mesh.shape["pair"], mesh.shape["aux"])

    def layer(*args):
        return body(sizes, *args)

    return jax.shard_map(
        layer,
        mesh=mesh,
        in_specs=placed,
        out_specs=P("pair", None, "aux"),
        check_vma=False,
    )
```

```python
import functools

import jax
import jax.numpy as jnp
from jax import lax
from jax.experimental import pallas as pl
from jax.experimental.pallas import tpu as pltpu
from jax.sharding import PartitionSpec as P


LANES = 128
BF = jnp.bfloat16
F32 = jnp.float32


def round_up(value, unit):
    return -(-value // unit) * unit


def flip(count, bits):
    return [(i, i ^ bits) for i in range(count)]


def member(aux, sides):
    return (aux // 2 % 2 if sides[1] == 2 else 0, aux % 2 if sides[0] == 2 else 0)


def prep_kernel(n_pair, sides, *refs):
    inputs, chunks, share_ref = refs[:6], refs[6 : 6 + n_pair], refs[6 + n_pair]
    buffers, (turned, sems) = refs[7 + n_pair : 13 + n_pair], refs[13 + n_pair :]
    copies = [
        pltpu.make_async_copy(src, dst, sems.at[i])
        for i, (src, dst) in enumerate(zip(inputs, buffers))
    ]
    for copy in copies:
        copy.start()
    panels, amps, lmo, near, ranks, fock = buffers
    local, rank, width = panels.shape
    part = width // n_pair
    wide = part // LANES
    rest = part - wide * LANES
    me = lax.axis_index("pair")
    aux = lax.axis_index("aux")
    slots = near.shape[1]
    for copy in copies[2:]:
        copy.wait()

    share_rows = share_ref.shape[0]
    row = lax.broadcasted_iota(jnp.int32, (16, LANES), 0)
    lane = lax.broadcasted_iota(jnp.int32, (16, LANES), 1)
    tail = jnp.zeros((16, LANES), F32)
    for lp in range(local):
        left, right = lmo[0, me * local + lp], lmo[1, me * local + lp]
        ids = [near[lp, k] for k in range(slots)]
        values = [fock[left, lmo[0, i]] + fock[right, lmo[1, i]] for i in ids]
        for k in range(slots):
            total = jnp.float32(0.0)
            fresh = jnp.float32(1.0)
            for j in range(slots):
                same = (ids[j] == ids[k]).astype(F32) if j != k else jnp.float32(1.0)
                total = total + same * values[j]
                if j < k:
                    fresh = fresh * (1.0 - same)
            here = lane == lp * slots + k
            tail = jnp.where(here & (row == 0), ids[k].astype(F32), tail)
            tail = jnp.where(here & (row == 1), total * fresh, tail)
    share_ref[share_rows - 16 :, :] = tail.astype(BF)

    freqs = amps.shape[1]
    many, take = local // sides[1], freqs // sides[0]
    lp_first, s_first = member(aux, sides)
    copies[1].wait()
    for i in range(many):
        for j in range(take):
            a = amps[lp_first * many + i, s_first * take + j].astype(F32)
            a = jnp.concatenate([a, jnp.zeros((rank, LANES - rank), F32)], axis=1)
            first = (i * take + j) * rank
            share_ref[first : first + rank, :] = a.astype(BF)

    copies[0].wait()
    for lp in range(local):
        keep = lax.broadcasted_iota(jnp.int32, (rank, LANES), 0) < ranks[lp]
        for k in range(n_pair):
            for w in range(wide):
                start = pl.multiple_of(((me ^ k) * wide + w) * LANES, LANES)
                x = panels[lp, :, pl.ds(start, LANES)].astype(F32)
                chunks[k][lp, w * rank : (w + 1) * rank, :] = jnp.where(keep, x, 0.0).astype(BF)
        if rest:
            for t in range(n_pair * rest // LANES):
                start = n_pair * wide * LANES + t * LANES
                x = panels[lp, :, start : start + LANES].astype(F32)
                x = jnp.where(keep, x, 0.0)
                x = jnp.concatenate([x, jnp.zeros((LANES - rank, LANES), F32)], axis=0)
                turned[t * LANES : (t + 1) * LANES, :] = x.T.astype(BF)
            for k in range(n_pair):
                start = pl.multiple_of((me ^ k) * rest, 16)
                chunks[k][lp, wide * rank :, :] = turned[pl.ds(start, rest), :]


def couple_kernel(n_pair, blocks, sides, shape, where, ids_ref, w_ref, *refs):
    half = n_pair // 2
    members = sides[0] * sides[1]
    panels, mats = list(refs[:n_pair]), refs[n_pair : n_pair + half * members]
    out_ref, proj, mixed, mat, own, sem = refs[n_pair + half * members :]
    local, rank, part, freqs = shape
    wide = part // LANES
    rest = part - wide * LANES
    rows = rank // blocks
    slots = ids_ref.shape[2]
    me, aux = where[0], where[1]
    many, take = local // sides[1], freqs // sides[0]
    copy = pltpu.make_async_copy(panels[0], own, sem)
    copy.start()
    panels[0] = own
    order = list(range(1, n_pair)) + [0]

    for k in order:
        if k == 0:
            copy.wait()
        for pair_slot in range(sides[1]):
            for i in range(many):
                lp = member(aux ^ (pair_slot * 2), sides)[0] * many + i
                for s in range(freqs):
                    slot, inner = s // take, s % take
                    first = (i * take + inner) * rank
                    piece = mats[(pair_slot * sides[0] + slot) * half + k % half]
                    mat[:, s * LANES : (s + 1) * LANES] = piece[k // half, first : first + rank, :]
                index = k * local + lp
                for w in range(wide):
                    proj[index, w * LANES : (w + 1) * LANES, :] = lax.dot_general(
                        panels[k][lp, w * rank : (w + 1) * rank, :],
                        mat[...],
                        (((0,), (0,)), ((), ())),
                        preferred_element_type=F32,
                    )
                if rest:
                    proj[index, wide * LANES :, :] = jnp.dot(
                        panels[k][lp, wide * rank :, :][:, :rank],
                        mat[...],
                        preferred_element_type=F32,
                    )

    tile = 32 if part % 32 == 0 else 16
    for k in order:
        for lp in range(local):
            source = []
            for j in range(slots):
                i = ids_ref[k, lp, j]
                source.append(((i // local) ^ me) * local + i % local)
            scale = [w_ref[k, lp, j] for j in range(slots)]
            for t in range(part // tile):
                span = slice(t * tile, (t + 1) * tile)
                acc = scale[0] * proj[source[0], span, :]
                for j in range(1, slots):
                    acc = acc + scale[j] * proj[source[j], span, :]
                mixed[span, :] = acc.astype(BF)
            got = None
            if wide:
                x = jnp.concatenate(
                    [panels[k][lp, w * rank : (w + 1) * rank, :] for w in range(wide)], axis=1
                )
                got = jnp.dot(x, mixed[: wide * LANES, :], preferred_element_type=F32)
            if rest:
                more = lax.dot_general(
                    panels[k][lp, wide * rank :, :],
                    mixed[wide * LANES :, :],
                    (((0,), (0,)), ((), ())),
                    preferred_element_type=F32,
                )[:rank]
                got = more if got is None else got + more
            for h in range(blocks):
                side = aux % 2 ^ (h % 2) if blocks > 1 else 0
                for s in range(freqs):
                    freq = member(aux ^ (s // take), sides)[1] * take + s % take
                    out_ref[side, me ^ k, h // 2, lp, freq, :rows, :] = got[
                        h * rows : (h + 1) * rows, s * LANES : (s + 1) * LANES
                    ].astype(out_ref.dtype)


def body(sizes, panels, amplitudes, drive, pno_energy, occ_energy, frequency, pair_lmo,
         neighbours, pno_ranks, fock_off):
    n_pair, n_aux = sizes
    local, rank, width = panels.shape
    freqs = amplitudes.shape[1]
    total = pair_lmo.shape[0]
    slots = neighbours.shape[1]
    even = rank % n_aux == 0 and n_aux % 2 == 0
    blocks = n_aux if even else 1
    rows = rank // blocks
    rows_pad = round_up(rows, 16)
    part = width // n_pair
    me_pair = lax.axis_index("pair")
    me_aux = lax.axis_index("aux")
    wide = part // LANES
    rest = part - wide * LANES
    chunk_rows = wide * rank + rest
    sides = (
        2 if n_aux % 2 == 0 and freqs % 2 == 0 else 1,
        2 if n_aux % 4 == 0 and freqs % 2 == 0 and local % 2 == 0 else 1,
    )
    where = jnp.stack([me_pair, me_aux]).astype(jnp.int32)
    vmem = pl.BlockSpec(memory_space=pltpu.VMEM)
    smem = pl.BlockSpec(memory_space=pltpu.SMEM)

    share_rows = (local // sides[1]) * (freqs // sides[0]) * rank + 16
    given = (panels, amplitudes, pair_lmo.T, neighbours, pno_ranks, fock_off)
    spaces = [pltpu.VMEM] * 2 + [pltpu.SMEM] * 4
    outs = pl.pallas_call(
        functools.partial(prep_kernel, n_pair, sides),
        out_shape=[jax.ShapeDtypeStruct((local, chunk_rows, LANES), BF)] * n_pair
        + [jax.ShapeDtypeStruct((share_rows, LANES), BF)],
        in_specs=[pl.BlockSpec(memory_space=pltpu.HBM)] * 6,
        out_specs=[vmem] * (n_pair + 1),
        scratch_shapes=[space(a.shape, a.dtype) for space, a in zip(spaces, given)]
        + [
            pltpu.VMEM((max(n_pair * rest, 16), LANES), BF),
            pltpu.SemaphoreType.DMA((6,)),
        ],
        cost_estimate=pl.CostEstimate(flops=0, bytes_accessed=4 * 2**20, transcendentals=0),
    )(*given)
    chunks, share = outs[:n_pair], outs[n_pair]

    far = n_pair // 2
    other = lax.ppermute(share, "pair", flip(n_pair, far))
    pieces = [jnp.concatenate([share[None], other[None]], axis=0)] + [None] * (far - 1)
    received = [chunks[0]] + [None] * (n_pair - 1)
    for k in range(1, n_pair):
        if k < far:
            pieces[k] = lax.ppermute(pieces[0], "pair", flip(n_pair, k))
        received[k] = lax.ppermute(chunks[k], "pair", flip(n_pair, k))
    tail = jnp.stack([piece[:, share_rows - 16 :] for piece in pieces], axis=1)
    tail = tail.reshape(n_pair, 16, LANES)
    ids = tail[:, 0, : local * slots].reshape(n_pair, local, slots).astype(jnp.int32)
    scale = tail[:, 1, : local * slots].reshape(n_pair, local, slots).astype(F32)
    if sides[1] == 2:
        for k in range(far):
            pieces.append(lax.ppermute(pieces[k], "aux", flip(n_aux, 2)))
    if sides[0] == 2:
        held, pieces = pieces, []
        for slot in range(sides[1]):
            block = held[slot * far : (slot + 1) * far]
            pieces += block
            for k in range(far):
                pieces.append(lax.ppermute(block[k], "aux", flip(n_aux, 1)))

    out_dims = (2 if even else 1, n_pair, max(blocks // 2, 1), local, freqs, rows_pad, LANES)
    flops = 4 * total * part * rank * freqs * LANES
    coupled = pl.pallas_call(
        functools.partial(
            couple_kernel, n_pair, blocks, sides, (local, rank, part, freqs)
        ),
        out_shape=jax.ShapeDtypeStruct(out_dims, BF if even else F32),
        in_specs=[smem] * 3
        + [pl.BlockSpec(memory_space=pltpu.HBM)]
        + [vmem] * (n_pair - 1 + far * sides[0] * sides[1]),
        out_specs=vmem,
        scratch_shapes=[
            pltpu.VMEM((total, part, freqs * LANES), F32),
            pltpu.VMEM((part, freqs * LANES), BF),
            pltpu.VMEM((rank, freqs * LANES), BF),
            pltpu.VMEM((local, chunk_rows, LANES), BF),
            pltpu.SemaphoreType.DMA,
        ],
        compiler_params=pltpu.CompilerParams(vmem_limit_bytes=40 * 2**20),
        cost_estimate=pl.CostEstimate(flops=flops, bytes_accessed=4 * 2**20, transcendentals=0),
    )(where, ids, scale, *received, *pieces)

    if even:
        other = lax.ppermute(coupled[1], "aux", flip(n_aux, 1))
        mine = (coupled[0].astype(F32) + other.astype(F32)).astype(BF)
        mine = mine.reshape((n_pair * (n_aux // 2),) + out_dims[3:])
        groups = [
            [g * n_aux + 2 * h + c for g in range(n_pair) for h in range(n_aux // 2)]
            for c in range(2)
        ]
        parts = lax.all_to_all(
            mine, ("pair", "aux"), 0, 0, axis_index_groups=groups, tiled=True
        )
        coupled_share = jnp.sum(parts.astype(F32), axis=0)[:, :, :rows, :rank].reshape(
            local, freqs, rows * rank
        )
    else:
        flat = coupled.reshape(total, freqs, rows_pad, LANES)[:, :, :rank, :rank]
        flat = flat.reshape(total, freqs, rank * rank)
        share_aux = lax.psum_scatter(flat, "aux", scatter_dimension=2, tiled=True)
        coupled_share = lax.psum_scatter(share_aux, "pair", scatter_dimension=0, tiled=True)

    share_width = drive.shape[2]
    start = me_aux * share_width
    lmo_ids = jnp.arange(occ_energy.shape[0], dtype=jnp.int32)
    own_lmo = lax.dynamic_slice_in_dim(pair_lmo, me_pair * local, local, 0)
    own_table = (own_lmo[:, :, None] == lmo_ids[None, None, :]).astype(F32)
    occ_pair = jnp.sum(own_table * occ_energy[None, None, :], axis=(1, 2))
    signs = jnp.array([1.0, -1.0], F32)
    if even:
        energy_rows = lax.dynamic_slice_in_dim(pno_energy, me_aux * rows, rows, 1)
        shift = energy_rows[:, :, None] + pno_energy[:, None, :] - occ_pair[:, None, None]
        factor = shift[:, None] - signs[None, :, None, None] * frequency[0]
        amp_rows_own = lax.dynamic_slice_in_dim(amplitudes, me_aux * rows, rows, 2)
        diagonal = (factor * amp_rows_own.astype(F32)).reshape(local, freqs, share_width)
    else:
        shift = pno_energy[:, :, None] + pno_energy[:, None, :] - occ_pair[:, None, None]
        factor = shift[:, None] - signs[None, :, None, None] * frequency[0]
        diagonal = (factor * amplitudes.astype(F32)).reshape(local, freqs, rank * rank)
        diagonal = lax.dynamic_slice_in_dim(diagonal, start, share_width, 2)
    return drive + diagonal + coupled_share


def solution(mesh):
    placed = (
        P("pair", None, "aux"),
        P("pair", None, None, None),
        P("pair", None, "aux"),
        P("pair", None),
        P(),
        P(),
        P(),
        P("pair", None),
        P("pair"),
        P(),
    )
    sizes = (mesh.shape["pair"], mesh.shape["aux"])

    def layer(*args):
        return body(sizes, *args)

    return jax.shard_map(
        layer,
        mesh=mesh,
        in_specs=placed,
        out_specs=P("pair", None, "aux"),
        check_vma=False,
    )
```

```python
import functools

import jax
import jax.numpy as jnp
from jax import lax
from jax.experimental import pallas as pl
from jax.experimental.pallas import tpu as pltpu
from jax.sharding import PartitionSpec as P


LANES = 128
BF = jnp.bfloat16
F32 = jnp.float32


def round_up(value, unit):
    return -(-value // unit) * unit


def flip(count, bits):
    return [(i, i ^ bits) for i in range(count)]


def member(aux, sides):
    return (aux // 2 % 2 if sides[1] == 2 else 0, aux % 2 if sides[0] == 2 else 0)


def prep_kernel(n_pair, sides, *refs):
    inputs, chunks, share_ref = refs[:6], refs[6], refs[7]
    buffers, (turned, sems) = refs[8:14], refs[14:]
    copies = [
        pltpu.make_async_copy(src, dst, sems.at[i])
        for i, (src, dst) in enumerate(zip(inputs, buffers))
    ]
    for copy in copies:
        copy.start()
    panels, amps, lmo, near, ranks, fock = buffers
    local, rank, width = panels.shape
    part = width // n_pair
    wide = part // LANES
    rest = part - wide * LANES
    me = lax.axis_index("pair")
    aux = lax.axis_index("aux")
    slots = near.shape[1]
    for copy in copies[2:]:
        copy.wait()

    share_rows = share_ref.shape[0]
    row = lax.broadcasted_iota(jnp.int32, (16, LANES), 0)
    lane = lax.broadcasted_iota(jnp.int32, (16, LANES), 1)
    tail = jnp.zeros((16, LANES), F32)
    for lp in range(local):
        left, right = lmo[0, me * local + lp], lmo[1, me * local + lp]
        ids = [near[lp, k] for k in range(slots)]
        values = [fock[left, lmo[0, i]] + fock[right, lmo[1, i]] for i in ids]
        for k in range(slots):
            total = jnp.float32(0.0)
            fresh = jnp.float32(1.0)
            for j in range(slots):
                same = (ids[j] == ids[k]).astype(F32) if j != k else jnp.float32(1.0)
                total = total + same * values[j]
                if j < k:
                    fresh = fresh * (1.0 - same)
            here = lane == lp * slots + k
            tail = jnp.where(here & (row == 0), ids[k].astype(F32), tail)
            tail = jnp.where(here & (row == 1), total * fresh, tail)
    share_ref[share_rows - 16 :, :] = tail.astype(BF)

    freqs = amps.shape[1]
    many, take = local // sides[1], freqs // sides[0]
    lp_first, s_first = member(aux, sides)
    copies[1].wait()
    for i in range(many):
        for j in range(take):
            a = amps[lp_first * many + i, s_first * take + j].astype(F32)
            a = jnp.concatenate([a, jnp.zeros((rank, LANES - rank), F32)], axis=1)
            first = (i * take + j) * rank
            share_ref[first : first + rank, :] = a.astype(BF)

    copies[0].wait()
    for lp in range(local):
        keep = lax.broadcasted_iota(jnp.int32, (rank, LANES), 0) < ranks[lp]
        for k in range(n_pair):
            for w in range(wide):
                start = pl.multiple_of(((me ^ k) * wide + w) * LANES, LANES)
                x = panels[lp, :, pl.ds(start, LANES)].astype(F32)
                chunks[me ^ k, lp, w * rank : (w + 1) * rank, :] = jnp.where(keep, x, 0.0).astype(BF)
        if rest:
            for t in range(n_pair * rest // LANES):
                start = n_pair * wide * LANES + t * LANES
                x = panels[lp, :, start : start + LANES].astype(F32)
                x = jnp.where(keep, x, 0.0)
                x = jnp.concatenate([x, jnp.zeros((LANES - rank, LANES), F32)], axis=0)
                turned[t * LANES : (t + 1) * LANES, :] = x.T.astype(BF)
            for k in range(n_pair):
                start = pl.multiple_of((me ^ k) * rest, 16)
                chunks[me ^ k, lp, wide * rank :, :] = turned[pl.ds(start, rest), :]


def couple_kernel(n_pair, blocks, sides, shape, where, ids_ref, w_ref, *refs):
    half = n_pair // 2
    members = sides[0] * sides[1]
    panels, mats = refs[0], refs[1 : 1 + half * members]
    out_ref, proj, mixed, mat = refs[1 + half * members :]
    local, rank, part, freqs = shape
    wide = part // LANES
    rest = part - wide * LANES
    rows = rank // blocks
    slots = ids_ref.shape[2]
    me, aux = where[0], where[1]
    many, take = local // sides[1], freqs // sides[0]
    order = list(range(n_pair))

    for k in order:
        for pair_slot in range(sides[1]):
            for i in range(many):
                lp = member(aux ^ (pair_slot * 2), sides)[0] * many + i
                for s in range(freqs):
                    slot, inner = s // take, s % take
                    first = (i * take + inner) * rank
                    piece = mats[(pair_slot * sides[0] + slot) * half + k % half]
                    mat[:, s * LANES : (s + 1) * LANES] = piece[k // half, first : first + rank, :]
                index = k * local + lp
                for w in range(wide):
                    proj[index, w * LANES : (w + 1) * LANES, :] = lax.dot_general(
                        panels[me ^ k, lp, w * rank : (w + 1) * rank, :],
                        mat[...],
                        (((0,), (0,)), ((), ())),
                        preferred_element_type=F32,
                    )
                if rest:
                    proj[index, wide * LANES :, :] = jnp.dot(
                        panels[me ^ k, lp, wide * rank :, :][:, :rank],
                        mat[...],
                        preferred_element_type=F32,
                    )

    tile = 32 if part % 32 == 0 else 16
    for k in order:
        for lp in range(local):
            source = []
            for j in range(slots):
                i = ids_ref[k, lp, j]
                source.append(((i // local) ^ me) * local + i % local)
            scale = [w_ref[k, lp, j] for j in range(slots)]
            for t in range(part // tile):
                span = slice(t * tile, (t + 1) * tile)
                acc = scale[0] * proj[source[0], span, :]
                for j in range(1, slots):
                    acc = acc + scale[j] * proj[source[j], span, :]
                mixed[span, :] = acc.astype(BF)
            got = None
            if wide:
                x = jnp.concatenate(
                    [panels[me ^ k, lp, w * rank : (w + 1) * rank, :] for w in range(wide)], axis=1
                )
                got = jnp.dot(x, mixed[: wide * LANES, :], preferred_element_type=F32)
            if rest:
                more = lax.dot_general(
                    panels[me ^ k, lp, wide * rank :, :],
                    mixed[wide * LANES :, :],
                    (((0,), (0,)), ((), ())),
                    preferred_element_type=F32,
                )[:rank]
                got = more if got is None else got + more
            for h in range(blocks):
                side = aux % 2 ^ (h % 2) if blocks > 1 else 0
                for s in range(freqs):
                    freq = member(aux ^ (s // take), sides)[1] * take + s % take
                    out_ref[side, me ^ k, h // 2, lp, freq, :rows, :] = got[
                        h * rows : (h + 1) * rows, s * LANES : (s + 1) * LANES
                    ].astype(out_ref.dtype)


def body(sizes, panels, amplitudes, drive, pno_energy, occ_energy, frequency, pair_lmo,
         neighbours, pno_ranks, fock_off):
    n_pair, n_aux = sizes
    local, rank, width = panels.shape
    freqs = amplitudes.shape[1]
    total = pair_lmo.shape[0]
    slots = neighbours.shape[1]
    even = rank % n_aux == 0 and n_aux % 2 == 0
    blocks = n_aux if even else 1
    rows = rank // blocks
    rows_pad = round_up(rows, 16)
    part = width // n_pair
    me_pair = lax.axis_index("pair")
    me_aux = lax.axis_index("aux")
    wide = part // LANES
    rest = part - wide * LANES
    chunk_rows = wide * rank + rest
    sides = (
        2 if n_aux % 2 == 0 and freqs % 2 == 0 else 1,
        1,
    )
    where = jnp.stack([me_pair, me_aux]).astype(jnp.int32)
    vmem = pl.BlockSpec(memory_space=pltpu.VMEM)
    smem = pl.BlockSpec(memory_space=pltpu.SMEM)

    share_rows = (local // sides[1]) * (freqs // sides[0]) * rank + 16
    given = (panels, amplitudes, pair_lmo.T, neighbours, pno_ranks, fock_off)
    spaces = [pltpu.VMEM] * 2 + [pltpu.SMEM] * 4
    outs = pl.pallas_call(
        functools.partial(prep_kernel, n_pair, sides),
        out_shape=[jax.ShapeDtypeStruct((n_pair, local, chunk_rows, LANES), BF)]
        + [jax.ShapeDtypeStruct((share_rows, LANES), BF)],
        in_specs=[pl.BlockSpec(memory_space=pltpu.HBM)] * 6,
        out_specs=[vmem] * 2,
        scratch_shapes=[space(a.shape, a.dtype) for space, a in zip(spaces, given)]
        + [
            pltpu.VMEM((max(n_pair * rest, 16), LANES), BF),
            pltpu.SemaphoreType.DMA((6,)),
        ],
        cost_estimate=pl.CostEstimate(flops=0, bytes_accessed=4 * 2**20, transcendentals=0),
    )(*given)
    chunks, share = outs

    far = n_pair // 2
    other = lax.ppermute(share, "pair", flip(n_pair, far))
    pieces = [jnp.concatenate([share[None], other[None]], axis=0)] + [None] * (far - 1)
    received = lax.all_to_all(chunks, "pair", 0, 0, tiled=True)
    for k in range(1, n_pair):
        if k < far:
            pieces[k] = lax.ppermute(pieces[0], "pair", flip(n_pair, k))
    tail = jnp.stack([piece[:, share_rows - 16 :] for piece in pieces], axis=1)
    tail = tail.reshape(n_pair, 16, LANES)
    ids = tail[:, 0, : local * slots].reshape(n_pair, local, slots).astype(jnp.int32)
    scale = tail[:, 1, : local * slots].reshape(n_pair, local, slots).astype(F32)
    if sides[1] == 2:
        for k in range(far):
            pieces.append(lax.ppermute(pieces[k], "aux", flip(n_aux, 2)))
    if sides[0] == 2:
        held, pieces = pieces, []
        for slot in range(sides[1]):
            block = held[slot * far : (slot + 1) * far]
            pieces += block
            for k in range(far):
                pieces.append(lax.ppermute(block[k], "aux", flip(n_aux, 1)))

    out_dims = (2 if even else 1, n_pair, max(blocks // 2, 1), local, freqs, rows_pad, LANES)
    flops = 4 * total * part * rank * freqs * LANES
    coupled = pl.pallas_call(
        functools.partial(
            couple_kernel, n_pair, blocks, sides, (local, rank, part, freqs)
        ),
        out_shape=jax.ShapeDtypeStruct(out_dims, BF if even else F32),
        in_specs=[smem] * 3
        + [vmem] * (1 + far * sides[0] * sides[1]),
        out_specs=vmem,
        scratch_shapes=[
            pltpu.VMEM((total, part, freqs * LANES), F32),
            pltpu.VMEM((part, freqs * LANES), BF),
            pltpu.VMEM((rank, freqs * LANES), BF),
        ],
        compiler_params=pltpu.CompilerParams(vmem_limit_bytes=40 * 2**20),
        cost_estimate=pl.CostEstimate(flops=flops, bytes_accessed=4 * 2**20, transcendentals=0),
    )(where, ids, scale, received, *pieces)

    if even:
        other = lax.ppermute(coupled[1], "aux", flip(n_aux, 1))
        mine = (coupled[0].astype(F32) + other.astype(F32)).astype(BF)
        mine = mine.reshape((n_pair * (n_aux // 2),) + out_dims[3:])
        groups = [
            [g * n_aux + 2 * h + c for g in range(n_pair) for h in range(n_aux // 2)]
            for c in range(2)
        ]
        parts = lax.all_to_all(
            mine, ("pair", "aux"), 0, 0, axis_index_groups=groups, tiled=True
        )
        coupled_share = jnp.sum(parts.astype(F32), axis=0)[:, :, :rows, :rank].reshape(
            local, freqs, rows * rank
        )
    else:
        flat = coupled.reshape(total, freqs, rows_pad, LANES)[:, :, :rank, :rank]
        flat = flat.reshape(total, freqs, rank * rank)
        share_aux = lax.psum_scatter(flat, "aux", scatter_dimension=2, tiled=True)
        coupled_share = lax.psum_scatter(share_aux, "pair", scatter_dimension=0, tiled=True)

    share_width = drive.shape[2]
    start = me_aux * share_width
    lmo_ids = jnp.arange(occ_energy.shape[0], dtype=jnp.int32)
    own_lmo = lax.dynamic_slice_in_dim(pair_lmo, me_pair * local, local, 0)
    own_table = (own_lmo[:, :, None] == lmo_ids[None, None, :]).astype(F32)
    occ_pair = jnp.sum(own_table * occ_energy[None, None, :], axis=(1, 2))
    signs = jnp.array([1.0, -1.0], F32)
    if even:
        energy_rows = lax.dynamic_slice_in_dim(pno_energy, me_aux * rows, rows, 1)
        shift = energy_rows[:, :, None] + pno_energy[:, None, :] - occ_pair[:, None, None]
        factor = shift[:, None] - signs[None, :, None, None] * frequency[0]
        amp_rows_own = lax.dynamic_slice_in_dim(amplitudes, me_aux * rows, rows, 2)
        diagonal = (factor * amp_rows_own.astype(F32)).reshape(local, freqs, share_width)
    else:
        shift = pno_energy[:, :, None] + pno_energy[:, None, :] - occ_pair[:, None, None]
        factor = shift[:, None] - signs[None, :, None, None] * frequency[0]
        diagonal = (factor * amplitudes.astype(F32)).reshape(local, freqs, rank * rank)
        diagonal = lax.dynamic_slice_in_dim(diagonal, start, share_width, 2)
    return drive + diagonal + coupled_share


def solution(mesh):
    placed = (
        P("pair", None, "aux"),
        P("pair", None, None, None),
        P("pair", None, "aux"),
        P("pair", None),
        P(),
        P(),
        P(),
        P("pair", None),
        P("pair"),
        P(),
    )
    sizes = (mesh.shape["pair"], mesh.shape["aux"])

    def layer(*args):
        return body(sizes, *args)

    return jax.shard_map(
        layer,
        mesh=mesh,
        in_specs=placed,
        out_specs=P("pair", None, "aux"),
        check_vma=False,
    )
```

```python
import functools

import jax
import jax.numpy as jnp
from jax import lax
from jax.experimental import pallas as pl
from jax.experimental.pallas import tpu as pltpu
from jax.sharding import PartitionSpec as P


LANES = 128
GROUP = 16
BF = jnp.bfloat16
F32 = jnp.float32


def round_up(value, unit):
    return -(-value // unit) * unit


def flip(count, bits):
    return [(i, i ^ bits) for i in range(count)]


def prep_kernel(n_pair, sides, *refs):
    inputs, chunks_out, share_out = refs[:6], refs[6], refs[7]
    buffers, (chunks, share_ref, turned, sems, panel_sems, out_sems) = refs[8:14], refs[14:]
    panels, amps, lmo, near, ranks, fock = buffers
    copies = [
        pltpu.make_async_copy(src, dst, sems.at[i])
        for i, (src, dst) in enumerate(zip(inputs[1:], buffers[1:]))
    ]
    panel_copies = [
        pltpu.make_async_copy(inputs[0].at[lp], panels.at[lp], panel_sems.at[lp])
        for lp in range(panels.shape[0])
    ]
    for copy in copies + panel_copies:
        copy.start()
    local, rank, width = panels.shape
    part = width // n_pair
    wide = part // LANES
    rest = part - wide * LANES
    me = lax.axis_index("pair")
    aux = lax.axis_index("aux")
    slots = near.shape[1]
    for copy in copies[1:]:
        copy.wait()

    share_rows = share_ref.shape[0]
    row = lax.broadcasted_iota(jnp.int32, (16, LANES), 0)
    lane = lax.broadcasted_iota(jnp.int32, (16, LANES), 1)
    tail = jnp.zeros((16, LANES), F32)
    for lp in range(local):
        left, right = lmo[0, me * local + lp], lmo[1, me * local + lp]
        ids = [near[lp, k] for k in range(slots)]
        values = [fock[left, lmo[0, i]] + fock[right, lmo[1, i]] for i in ids]
        for k in range(slots):
            total = jnp.float32(0.0)
            fresh = jnp.float32(1.0)
            for j in range(slots):
                same = (ids[j] == ids[k]).astype(F32) if j != k else jnp.float32(1.0)
                total = total + same * values[j]
                if j < k:
                    fresh = fresh * (1.0 - same)
            here = lane == lp * slots + k
            tail = jnp.where(here & (row == 0), ids[k].astype(F32), tail)
            tail = jnp.where(here & (row == 1), total * fresh, tail)
    share_ref[share_rows - 16 :, :] = tail.astype(BF)

    freqs = amps.shape[1]
    take = freqs // sides
    s_first = aux % 2 if sides == 2 else 0
    copies[0].wait()
    for i in range(local):
        for j in range(take):
            a = amps[i, s_first * take + j].astype(F32)
            a = jnp.concatenate([a, jnp.zeros((rank, LANES - rank), F32)], axis=1)
            first = (i * take + j) * rank
            share_ref[first : first + rank, :] = a.astype(BF)

    sends = [pltpu.make_async_copy(share_ref, share_out, out_sems.at[local])]
    sends[0].start()
    for lp in range(local):
        panel_copies[lp].wait()
        keep = lax.broadcasted_iota(jnp.int32, (rank, LANES), 0) < ranks[lp]
        for k in range(n_pair):
            for w in range(wide):
                start = pl.multiple_of(((me ^ k) * wide + w) * LANES, LANES)
                x = panels[lp, :, pl.ds(start, LANES)].astype(F32)
                chunks[me ^ k, lp, w * rank : (w + 1) * rank, :] = jnp.where(keep, x, 0.0).astype(BF)
        if rest:
            for t in range(n_pair * rest // LANES):
                start = n_pair * wide * LANES + t * LANES
                x = panels[lp, :, start : start + LANES].astype(F32)
                x = jnp.where(keep, x, 0.0)
                x = jnp.concatenate([x, jnp.zeros((LANES - rank, LANES), F32)], axis=0)
                turned[lp, t * LANES : (t + 1) * LANES, :] = x.T.astype(BF)
            for k in range(n_pair):
                start = pl.multiple_of((me ^ k) * rest, 16)
                chunks[me ^ k, lp, wide * rank :, :] = turned[lp, pl.ds(start, rest), :]
        send = pltpu.make_async_copy(chunks.at[:, lp], chunks_out.at[:, lp], out_sems.at[lp])
        send.start()
        sends.append(send)
    for send in sends:
        send.wait()


def mix_kernel(local, where, ids_ref, w_ref, out_ref):
    n_pair, slots = ids_ref.shape[0], ids_ref.shape[2]
    me = where[0]
    side = out_ref.shape[1]
    group = lax.broadcasted_iota(jnp.int32, (GROUP, side), 1) // GROUP
    inner = lax.broadcasted_iota(jnp.int32, (GROUP, side), 1) % GROUP
    diagonal = lax.broadcasted_iota(jnp.int32, (GROUP, side), 0) == inner
    for k in range(n_pair):
        for lp in range(local):
            acc = jnp.zeros((GROUP, side), F32)
            for j in range(slots):
                i = ids_ref[k, lp, j]
                source = ((i // local) ^ me) * local + i % local
                acc = acc + jnp.where(group == source, w_ref[k, lp, j], 0.0)
            first = (k * local + lp) * GROUP
            out_ref[first : first + GROUP, :] = jnp.where(diagonal, acc, 0.0).astype(BF)


def couple_kernel(n_pair, blocks, sides, shape, where, panels, mix_ref, *refs):
    half = n_pair // 2
    mats = refs[: half * sides]
    out_ref, proj, mixed, mat = refs[half * sides :]
    local, rank, part, freqs = shape
    total = n_pair * local
    wide = part // LANES
    rest = part - wide * LANES
    rows = rank // blocks
    lanes = freqs * LANES
    me, aux = where[0], where[1]
    take = freqs // sides

    def keep(first, index, value):
        count = value.shape[0] // GROUP
        proj[first // GROUP : first // GROUP + count, index] = value.astype(BF).reshape(
            count, GROUP, lanes
        )

    for k in range(n_pair):
        for lp in range(local):
            index = k * local + lp
            for s in range(freqs):
                slot, inner = s // take, s % take
                first = (lp * take + inner) * rank
                piece = mats[slot * half + k % half].at[k // half]
                mat[index, :, s * LANES : (s + 1) * LANES] = piece[first : first + rank, :]
            for w in range(wide):
                found = lax.dot_general(
                    panels[me ^ k, lp, w * rank : (w + 1) * rank, :],
                    mat[index],
                    (((0,), (0,)), ((), ())),
                    preferred_element_type=F32,
                )
                keep(w * LANES, index, found)
            if rest:
                found = jnp.dot(
                    panels[me ^ k, lp, wide * rank :, :][:, :rank],
                    mat[index],
                    preferred_element_type=F32,
                )
                keep(wide * LANES, index, found)

    for g in range(part // GROUP):
        found = jnp.dot(
            mix_ref[...], proj[g].reshape(total * GROUP, lanes), preferred_element_type=F32
        )
        mixed[:, g * GROUP : (g + 1) * GROUP, :] = found.astype(BF).reshape(total, GROUP, lanes)

    for k in range(n_pair):
        for lp in range(local):
            index = k * local + lp
            got = None
            if wide:
                x = jnp.concatenate(
                    [panels[me ^ k, lp, w * rank : (w + 1) * rank, :] for w in range(wide)], axis=1
                )
                got = jnp.dot(x, mixed[index, : wide * LANES, :], preferred_element_type=F32)
            if rest:
                more = lax.dot_general(
                    panels[me ^ k, lp, wide * rank :, :],
                    mixed[index, wide * LANES :, :],
                    (((0,), (0,)), ((), ())),
                    preferred_element_type=F32,
                )[:rank]
                got = more if got is None else got + more
            for h in range(blocks):
                side = aux % 2 ^ (h % 2) if blocks > 1 else 0
                for s in range(freqs):
                    freq = (s // take ^ (aux % 2)) * take + s % take if sides == 2 else s
                    out_ref[side, me ^ k, h // 2, lp, freq, :rows, :] = got[
                        h * rows : (h + 1) * rows, s * LANES : (s + 1) * LANES
                    ].astype(out_ref.dtype)


def body(sizes, panels, amplitudes, drive, pno_energy, occ_energy, frequency, pair_lmo,
         neighbours, pno_ranks, fock_off):
    n_pair, n_aux = sizes
    local, rank, width = panels.shape
    freqs = amplitudes.shape[1]
    total = pair_lmo.shape[0]
    slots = neighbours.shape[1]
    even = rank % n_aux == 0 and n_aux % 2 == 0
    blocks = n_aux if even else 1
    rows = rank // blocks
    rows_pad = round_up(rows, 16)
    part = width // n_pair
    me_pair = lax.axis_index("pair")
    me_aux = lax.axis_index("aux")
    wide = part // LANES
    rest = part - wide * LANES
    chunk_rows = wide * rank + rest
    sides = 2 if n_aux % 2 == 0 and freqs % 2 == 0 else 1
    where = jnp.stack([me_pair, me_aux]).astype(jnp.int32)
    vmem = pl.BlockSpec(memory_space=pltpu.VMEM)
    smem = pl.BlockSpec(memory_space=pltpu.SMEM)

    share_rows = local * (freqs // sides) * rank + 16
    given = (panels, amplitudes, pair_lmo.T, neighbours, pno_ranks, fock_off)
    spaces = [pltpu.VMEM] * 2 + [pltpu.SMEM] * 4
    outs = pl.pallas_call(
        functools.partial(prep_kernel, n_pair, sides),
        out_shape=[jax.ShapeDtypeStruct((n_pair, local, chunk_rows, LANES), BF)]
        + [jax.ShapeDtypeStruct((share_rows, LANES), BF)],
        in_specs=[pl.BlockSpec(memory_space=pltpu.HBM)] * 6,
        out_specs=[pl.BlockSpec(memory_space=pltpu.HBM)] * 2,
        scratch_shapes=[space(a.shape, a.dtype) for space, a in zip(spaces, given)]
        + [
            pltpu.VMEM((n_pair, local, chunk_rows, LANES), BF),
            pltpu.VMEM((share_rows, LANES), BF),
            pltpu.VMEM((local, max(n_pair * rest, 16), LANES), BF),
            pltpu.SemaphoreType.DMA((5,)),
            pltpu.SemaphoreType.DMA((local,)),
            pltpu.SemaphoreType.DMA((local + 1,)),
        ],
        cost_estimate=pl.CostEstimate(flops=0, bytes_accessed=4 * 2**20, transcendentals=0),
    )(*given)
    chunks, share = outs

    far = n_pair // 2
    other = lax.ppermute(share, "pair", flip(n_pair, far))
    pieces = [jnp.concatenate([share[None], other[None]], axis=0)] + [None] * (far - 1)
    received = lax.all_to_all(chunks, "pair", 0, 0, tiled=True)
    for k in range(1, n_pair):
        if k < far:
            pieces[k] = lax.ppermute(pieces[0], "pair", flip(n_pair, k))
    tail = jnp.stack([piece[:, share_rows - 16 :] for piece in pieces], axis=1)
    tail = tail.reshape(n_pair, 16, LANES)
    ids = tail[:, 0, : local * slots].reshape(n_pair, local, slots).astype(jnp.int32)
    scale = tail[:, 1, : local * slots].reshape(n_pair, local, slots).astype(F32)
    if sides == 2:
        for k in range(far):
            pieces.append(lax.ppermute(pieces[k], "aux", flip(n_aux, 1)))
    mix = pl.pallas_call(
        functools.partial(mix_kernel, local),
        out_shape=jax.ShapeDtypeStruct((total * GROUP, total * GROUP), BF),
        in_specs=[smem] * 3,
        out_specs=vmem,
        compiler_params=pltpu.CompilerParams(vmem_limit_bytes=8 * 2**20),
        cost_estimate=pl.CostEstimate(flops=10**6, bytes_accessed=2**17, transcendentals=0),
    )(where, ids, scale)

    out_dims = (2 if even else 1, n_pair, max(blocks // 2, 1), local, freqs, rows_pad, LANES)
    flops = 4 * total * part * rank * freqs * LANES
    coupled = pl.pallas_call(
        functools.partial(
            couple_kernel, n_pair, blocks, sides, (local, rank, part, freqs)
        ),
        out_shape=jax.ShapeDtypeStruct(out_dims, BF if even else F32),
        in_specs=[smem] + [vmem] * (2 + far * sides),
        out_specs=vmem,
        scratch_shapes=[
            pltpu.VMEM((part // GROUP, total, GROUP, freqs * LANES), BF),
            pltpu.VMEM((total, part, freqs * LANES), BF),
            pltpu.VMEM((total, rank, freqs * LANES), BF),
        ],
        compiler_params=pltpu.CompilerParams(vmem_limit_bytes=40 * 2**20),
        cost_estimate=pl.CostEstimate(flops=flops, bytes_accessed=4 * 2**20, transcendentals=0),
    )(where, received, mix, *pieces)

    if even:
        other = lax.ppermute(coupled[1], "aux", flip(n_aux, 1))
        mine = (coupled[0].astype(F32) + other.astype(F32)).astype(BF)
        mine = mine.reshape((n_pair * (n_aux // 2),) + out_dims[3:])
        groups = [
            [g * n_aux + 2 * h + c for g in range(n_pair) for h in range(n_aux // 2)]
            for c in range(2)
        ]
        parts = lax.all_to_all(
            mine, ("pair", "aux"), 0, 0, axis_index_groups=groups, tiled=True
        )
        coupled_share = jnp.sum(parts.astype(F32), axis=0)[:, :, :rows, :rank].reshape(
            local, freqs, rows * rank
        )
    else:
        flat = coupled.reshape(total, freqs, rows_pad, LANES)[:, :, :rank, :rank]
        flat = flat.reshape(total, freqs, rank * rank)
        share_aux = lax.psum_scatter(flat, "aux", scatter_dimension=2, tiled=True)
        coupled_share = lax.psum_scatter(share_aux, "pair", scatter_dimension=0, tiled=True)

    share_width = drive.shape[2]
    start = me_aux * share_width
    lmo_ids = jnp.arange(occ_energy.shape[0], dtype=jnp.int32)
    own_lmo = lax.dynamic_slice_in_dim(pair_lmo, me_pair * local, local, 0)
    own_table = (own_lmo[:, :, None] == lmo_ids[None, None, :]).astype(F32)
    occ_pair = jnp.sum(own_table * occ_energy[None, None, :], axis=(1, 2))
    signs = jnp.array([1.0, -1.0], F32)
    if even:
        energy_rows = lax.dynamic_slice_in_dim(pno_energy, me_aux * rows, rows, 1)
        shift = energy_rows[:, :, None] + pno_energy[:, None, :] - occ_pair[:, None, None]
        factor = shift[:, None] - signs[None, :, None, None] * frequency[0]
        amp_rows_own = lax.dynamic_slice_in_dim(amplitudes, me_aux * rows, rows, 2)
        diagonal = (factor * amp_rows_own.astype(F32)).reshape(local, freqs, share_width)
    else:
        shift = pno_energy[:, :, None] + pno_energy[:, None, :] - occ_pair[:, None, None]
        factor = shift[:, None] - signs[None, :, None, None] * frequency[0]
        diagonal = (factor * amplitudes.astype(F32)).reshape(local, freqs, rank * rank)
        diagonal = lax.dynamic_slice_in_dim(diagonal, start, share_width, 2)
    return drive + diagonal + coupled_share


def solution(mesh):
    placed = (
        P("pair", None, "aux"),
        P("pair", None, None, None),
        P("pair", None, "aux"),
        P("pair", None),
        P(),
        P(),
        P(),
        P("pair", None),
        P("pair"),
        P(),
    )
    sizes = (mesh.shape["pair"], mesh.shape["aux"])

    def layer(*args):
        return body(sizes, *args)

    return jax.shard_map(
        layer,
        mesh=mesh,
        in_specs=placed,
        out_specs=P("pair", None, "aux"),
        check_vma=False,
    )
```

```python
import functools

import jax
import jax.numpy as jnp
from jax import lax
from jax.experimental import pallas as pl
from jax.experimental.pallas import tpu as pltpu
from jax.sharding import PartitionSpec as P


LANES = 128
GROUP = 16
BF = jnp.bfloat16
F32 = jnp.float32


def round_up(value, unit):
    return -(-value // unit) * unit


def flip(count, bits):
    return [(i, i ^ bits) for i in range(count)]


def prep_kernel(n_pair, sides, *refs):
    inputs, chunks_out, share_out = refs[:6], refs[6], refs[7]
    buffers, (chunks, share_ref, turned, sems, panel_sems, out_sems) = refs[8:14], refs[14:]
    panels, amps, lmo, near, ranks, fock = buffers
    copies = [
        pltpu.make_async_copy(src, dst, sems.at[i])
        for i, (src, dst) in enumerate(zip(inputs[1:], buffers[1:]))
    ]
    panel_copies = [
        pltpu.make_async_copy(inputs[0].at[lp], panels.at[lp], panel_sems.at[lp])
        for lp in range(panels.shape[0])
    ]
    for copy in copies + panel_copies:
        copy.start()
    local, rank, width = panels.shape
    part = width // n_pair
    wide = part // LANES
    rest = part - wide * LANES
    me = lax.axis_index("pair")
    aux = lax.axis_index("aux")
    slots = near.shape[1]
    for copy in copies[1:]:
        copy.wait()

    share_rows = share_ref.shape[0]
    row = lax.broadcasted_iota(jnp.int32, (16, LANES), 0)
    lane = lax.broadcasted_iota(jnp.int32, (16, LANES), 1)
    tail = jnp.zeros((16, LANES), F32)
    for lp in range(local):
        left, right = lmo[0, me * local + lp], lmo[1, me * local + lp]
        ids = [near[lp, k] for k in range(slots)]
        values = [fock[left, lmo[0, i]] + fock[right, lmo[1, i]] for i in ids]
        for k in range(slots):
            total = jnp.float32(0.0)
            fresh = jnp.float32(1.0)
            for j in range(slots):
                same = (ids[j] == ids[k]).astype(F32) if j != k else jnp.float32(1.0)
                total = total + same * values[j]
                if j < k:
                    fresh = fresh * (1.0 - same)
            here = lane == lp * slots + k
            tail = jnp.where(here & (row == 0), ids[k].astype(F32), tail)
            tail = jnp.where(here & (row == 1), total * fresh, tail)
    share_ref[share_rows - 16 :, :] = tail.astype(BF)

    freqs = amps.shape[1]
    take = freqs // sides
    s_first = aux % 2 if sides == 2 else 0
    copies[0].wait()
    for i in range(local):
        for j in range(take):
            a = amps[i, s_first * take + j].astype(F32)
            a = jnp.concatenate([a, jnp.zeros((rank, LANES - rank), F32)], axis=1)
            first = (i * take + j) * rank
            share_ref[first : first + rank, :] = a.astype(BF)

    sends = [pltpu.make_async_copy(share_ref, share_out, out_sems.at[local])]
    sends[0].start()
    for lp in range(local):
        panel_copies[lp].wait()
        keep = lax.broadcasted_iota(jnp.int32, (rank, LANES), 0) < ranks[lp]
        for k in range(n_pair):
            for w in range(wide):
                start = pl.multiple_of(((me ^ k) * wide + w) * LANES, LANES)
                x = panels[lp, :, pl.ds(start, LANES)].astype(F32)
                chunks[me ^ k, lp, w * rank : (w + 1) * rank, :] = jnp.where(keep, x, 0.0).astype(BF)
        if rest:
            for t in range(n_pair * rest // LANES):
                start = n_pair * wide * LANES + t * LANES
                x = panels[lp, :, start : start + LANES].astype(F32)
                x = jnp.where(keep, x, 0.0)
                x = jnp.concatenate([x, jnp.zeros((LANES - rank, LANES), F32)], axis=0)
                turned[lp, t * LANES : (t + 1) * LANES, :] = x.T.astype(BF)
            for k in range(n_pair):
                start = pl.multiple_of((me ^ k) * rest, 16)
                chunks[me ^ k, lp, wide * rank :, :] = turned[lp, pl.ds(start, rest), :]
        send = pltpu.make_async_copy(chunks.at[:, lp], chunks_out.at[:, lp], out_sems.at[lp])
        send.start()
        sends.append(send)
    for send in sends:
        send.wait()


def couple_kernel(n_pair, blocks, sides, shape, table, panels, *refs):
    half = n_pair // 2
    mats = refs[: half * sides]
    out_ref, proj, mixed, mat, mix_ref = refs[half * sides :]
    local, rank, part, freqs = shape
    total = n_pair * local
    wide = part // LANES
    rest = part - wide * LANES
    rows = rank // blocks
    lanes = freqs * LANES
    me, aux = lax.axis_index("pair"), lax.axis_index("aux")
    take = freqs // sides

    def keep(first, index, value):
        count = value.shape[0] // GROUP
        proj[first // GROUP : first // GROUP + count, index] = value.astype(BF).reshape(
            count, GROUP, lanes
        )

    half_group = GROUP // 2
    lane = lax.broadcasted_iota(jnp.int32, (half_group, total * GROUP), 1)
    row = lax.broadcasted_iota(jnp.int32, (half_group, total * GROUP), 0)
    column = lane % GROUP
    group = lane // GROUP
    group = (((group // local) ^ me) * local + group % local).astype(F32)
    slots = table.shape[2] // local

    for k in range(n_pair):
        for lp in range(local):
            index = k * local + lp
            acc = jnp.zeros((half_group, total * GROUP), F32)
            for j in range(lp * slots, (lp + 1) * slots):
                acc = acc + jnp.where(group == table[k, 0, j], table[k, 1, j], 0.0)
            both = [
                jnp.where(column == row + shift, acc, 0.0) for shift in (0, half_group)
            ]
            mix_ref[index * GROUP : (index + 1) * GROUP, :] = jnp.concatenate(both, axis=0).astype(
                BF
            )
            for s in range(freqs):
                slot, inner = s // take, s % take
                first = (lp * take + inner) * rank
                piece = mats[slot * half + k % half].at[k // half]
                mat[index, :, s * LANES : (s + 1) * LANES] = piece[first : first + rank, :]
            for w in range(wide):
                found = lax.dot_general(
                    panels[me ^ k, lp, w * rank : (w + 1) * rank, :],
                    mat[index],
                    (((0,), (0,)), ((), ())),
                    preferred_element_type=F32,
                )
                keep(w * LANES, index, found)
            if rest:
                found = jnp.dot(
                    panels[me ^ k, lp, wide * rank :, :][:, :rank],
                    mat[index],
                    preferred_element_type=F32,
                )
                keep(wide * LANES, index, found)

    for g in range(part // GROUP):
        found = jnp.dot(
            mix_ref[...], proj[g].reshape(total * GROUP, lanes), preferred_element_type=F32
        )
        mixed[:, g * GROUP : (g + 1) * GROUP, :] = found.astype(BF).reshape(total, GROUP, lanes)

    for k in range(n_pair):
        for lp in range(local):
            index = k * local + lp
            got = None
            if wide:
                x = jnp.concatenate(
                    [panels[me ^ k, lp, w * rank : (w + 1) * rank, :] for w in range(wide)], axis=1
                )
                got = jnp.dot(x, mixed[index, : wide * LANES, :], preferred_element_type=F32)
            if rest:
                more = lax.dot_general(
                    panels[me ^ k, lp, wide * rank :, :],
                    mixed[index, wide * LANES :, :],
                    (((0,), (0,)), ((), ())),
                    preferred_element_type=F32,
                )[:rank]
                got = more if got is None else got + more
            for h in range(blocks):
                side = aux % 2 ^ (h % 2) if blocks > 1 else 0
                for s in range(freqs):
                    freq = (s // take ^ (aux % 2)) * take + s % take if sides == 2 else s
                    out_ref[side, me ^ k, h // 2, lp, freq, :rows, :] = got[
                        h * rows : (h + 1) * rows, s * LANES : (s + 1) * LANES
                    ].astype(out_ref.dtype)


def body(sizes, panels, amplitudes, drive, pno_energy, occ_energy, frequency, pair_lmo,
         neighbours, pno_ranks, fock_off):
    n_pair, n_aux = sizes
    local, rank, width = panels.shape
    freqs = amplitudes.shape[1]
    total = pair_lmo.shape[0]
    slots = neighbours.shape[1]
    even = rank % n_aux == 0 and n_aux % 2 == 0
    blocks = n_aux if even else 1
    rows = rank // blocks
    rows_pad = round_up(rows, 16)
    part = width // n_pair
    me_pair = lax.axis_index("pair")
    me_aux = lax.axis_index("aux")
    wide = part // LANES
    rest = part - wide * LANES
    chunk_rows = wide * rank + rest
    sides = 2 if n_aux % 2 == 0 and freqs % 2 == 0 else 1
    vmem = pl.BlockSpec(memory_space=pltpu.VMEM)
    smem = pl.BlockSpec(memory_space=pltpu.SMEM)

    share_rows = local * (freqs // sides) * rank + 16
    given = (panels, amplitudes, pair_lmo.T, neighbours, pno_ranks, fock_off)
    spaces = [pltpu.VMEM] * 2 + [pltpu.SMEM] * 4
    outs = pl.pallas_call(
        functools.partial(prep_kernel, n_pair, sides),
        out_shape=[jax.ShapeDtypeStruct((n_pair, local, chunk_rows, LANES), BF)]
        + [jax.ShapeDtypeStruct((share_rows, LANES), BF)],
        in_specs=[pl.BlockSpec(memory_space=pltpu.HBM)] * 6,
        out_specs=[pl.BlockSpec(memory_space=pltpu.HBM)] * 2,
        scratch_shapes=[space(a.shape, a.dtype) for space, a in zip(spaces, given)]
        + [
            pltpu.VMEM((n_pair, local, chunk_rows, LANES), BF),
            pltpu.VMEM((share_rows, LANES), BF),
            pltpu.VMEM((local, max(n_pair * rest, 16), LANES), BF),
            pltpu.SemaphoreType.DMA((5,)),
            pltpu.SemaphoreType.DMA((local,)),
            pltpu.SemaphoreType.DMA((local + 1,)),
        ],
        cost_estimate=pl.CostEstimate(flops=0, bytes_accessed=4 * 2**20, transcendentals=0),
    )(*given)
    chunks, share = outs

    far = n_pair // 2
    other = lax.ppermute(share, "pair", flip(n_pair, far))
    pieces = [jnp.concatenate([share[None], other[None]], axis=0)] + [None] * (far - 1)
    received = lax.all_to_all(chunks, "pair", 0, 0, tiled=True)
    for k in range(1, n_pair):
        if k < far:
            pieces[k] = lax.ppermute(pieces[0], "pair", flip(n_pair, k))
    tail = jnp.stack([piece[:, share_rows - 16 :] for piece in pieces], axis=1)
    table = tail.reshape(n_pair, 16, LANES)[:, :2, : local * slots].astype(F32)
    if sides == 2:
        for k in range(far):
            pieces.append(lax.ppermute(pieces[k], "aux", flip(n_aux, 1)))
    out_dims = (2 if even else 1, n_pair, max(blocks // 2, 1), local, freqs, rows_pad, LANES)
    flops = 4 * total * part * rank * freqs * LANES
    coupled = pl.pallas_call(
        functools.partial(
            couple_kernel, n_pair, blocks, sides, (local, rank, part, freqs)
        ),
        out_shape=jax.ShapeDtypeStruct(out_dims, BF if even else F32),
        in_specs=[smem] + [vmem] * (1 + far * sides),
        out_specs=vmem,
        scratch_shapes=[
            pltpu.VMEM((part // GROUP, total, GROUP, freqs * LANES), BF),
            pltpu.VMEM((total, part, freqs * LANES), BF),
            pltpu.VMEM((total, rank, freqs * LANES), BF),
            pltpu.VMEM((total * GROUP, total * GROUP), BF),
        ],
        compiler_params=pltpu.CompilerParams(vmem_limit_bytes=40 * 2**20),
        cost_estimate=pl.CostEstimate(flops=flops, bytes_accessed=4 * 2**20, transcendentals=0),
    )(table, received, *pieces)

    if even:
        other = lax.ppermute(coupled[1], "aux", flip(n_aux, 1))
        mine = (coupled[0].astype(F32) + other.astype(F32)).astype(BF)
        mine = mine.reshape((n_pair * (n_aux // 2),) + out_dims[3:])
        groups = [
            [g * n_aux + 2 * h + c for g in range(n_pair) for h in range(n_aux // 2)]
            for c in range(2)
        ]
        parts = lax.all_to_all(
            mine, ("pair", "aux"), 0, 0, axis_index_groups=groups, tiled=True
        )
        coupled_share = jnp.sum(parts.astype(F32), axis=0)[:, :, :rows, :rank].reshape(
            local, freqs, rows * rank
        )
    else:
        flat = coupled.reshape(total, freqs, rows_pad, LANES)[:, :, :rank, :rank]
        flat = flat.reshape(total, freqs, rank * rank)
        share_aux = lax.psum_scatter(flat, "aux", scatter_dimension=2, tiled=True)
        coupled_share = lax.psum_scatter(share_aux, "pair", scatter_dimension=0, tiled=True)

    share_width = drive.shape[2]
    start = me_aux * share_width
    lmo_ids = jnp.arange(occ_energy.shape[0], dtype=jnp.int32)
    own_lmo = lax.dynamic_slice_in_dim(pair_lmo, me_pair * local, local, 0)
    own_table = (own_lmo[:, :, None] == lmo_ids[None, None, :]).astype(F32)
    occ_pair = jnp.sum(own_table * occ_energy[None, None, :], axis=(1, 2))
    signs = jnp.array([1.0, -1.0], F32)
    if even:
        energy_rows = lax.dynamic_slice_in_dim(pno_energy, me_aux * rows, rows, 1)
        shift = energy_rows[:, :, None] + pno_energy[:, None, :] - occ_pair[:, None, None]
        factor = shift[:, None] - signs[None, :, None, None] * frequency[0]
        amp_rows_own = lax.dynamic_slice_in_dim(amplitudes, me_aux * rows, rows, 2)
        diagonal = (factor * amp_rows_own.astype(F32)).reshape(local, freqs, share_width)
    else:
        shift = pno_energy[:, :, None] + pno_energy[:, None, :] - occ_pair[:, None, None]
        factor = shift[:, None] - signs[None, :, None, None] * frequency[0]
        diagonal = (factor * amplitudes.astype(F32)).reshape(local, freqs, rank * rank)
        diagonal = lax.dynamic_slice_in_dim(diagonal, start, share_width, 2)
    return drive + diagonal + coupled_share


def solution(mesh):
    placed = (
        P("pair", None, "aux"),
        P("pair", None, None, None),
        P("pair", None, "aux"),
        P("pair", None),
        P(),
        P(),
        P(),
        P("pair", None),
        P("pair"),
        P(),
    )
    sizes = (mesh.shape["pair"], mesh.shape["aux"])

    def layer(*args):
        return body(sizes, *args)

    return jax.shard_map(
        layer,
        mesh=mesh,
        in_specs=placed,
        out_specs=P("pair", None, "aux"),
        check_vma=False,
    )
```

```python
import functools

import jax
import jax.numpy as jnp
from jax import lax
from jax.experimental import pallas as pl
from jax.experimental.pallas import tpu as pltpu
from jax.sharding import PartitionSpec as P


LANES = 128
GROUP = 16
BF = jnp.bfloat16
F32 = jnp.float32


def flip(count, bits):
    return [(i, i ^ bits) for i in range(count)]


def prep_kernel(n_pair, sides, *refs):
    inputs, chunks_out, share_out = refs[:6], refs[6], refs[7]
    buffers, (chunks, share_ref, turned, sems, panel_sems, out_sems) = refs[8:14], refs[14:]
    panels, amps, lmo, near, ranks, fock = buffers
    copies = [
        pltpu.make_async_copy(src, dst, sems.at[i])
        for i, (src, dst) in enumerate(zip(inputs[1:], buffers[1:]))
    ]
    panel_copies = [
        pltpu.make_async_copy(inputs[0].at[lp], panels.at[lp], panel_sems.at[lp])
        for lp in range(panels.shape[0])
    ]
    for copy in copies + panel_copies:
        copy.start()
    local, rank, width = panels.shape
    part = width // n_pair
    wide = part // LANES
    rest = part - wide * LANES
    me = lax.axis_index("pair")
    aux = lax.axis_index("aux")
    slots = near.shape[1]
    for copy in copies[1:]:
        copy.wait()

    share_rows = share_ref.shape[0]
    row = lax.broadcasted_iota(jnp.int32, (16, LANES), 0)
    lane = lax.broadcasted_iota(jnp.int32, (16, LANES), 1)
    tail = jnp.zeros((16, LANES), F32)
    for lp in range(local):
        left, right = lmo[0, me * local + lp], lmo[1, me * local + lp]
        ids = [near[lp, k] for k in range(slots)]
        values = [fock[left, lmo[0, i]] + fock[right, lmo[1, i]] for i in ids]
        for k in range(slots):
            total = jnp.float32(0.0)
            fresh = jnp.float32(1.0)
            for j in range(slots):
                same = (ids[j] == ids[k]).astype(F32) if j != k else jnp.float32(1.0)
                total = total + same * values[j]
                if j < k:
                    fresh = fresh * (1.0 - same)
            here = lane == lp * slots + k
            tail = jnp.where(here & (row == 0), ids[k].astype(F32), tail)
            tail = jnp.where(here & (row == 1), total * fresh, tail)
    share_ref[share_rows - 16 :, :] = tail.astype(BF)

    freqs = amps.shape[1]
    take = freqs // sides
    s_first = aux % 2 if sides == 2 else 0
    copies[0].wait()
    for i in range(local):
        for j in range(take):
            a = amps[i, s_first * take + j].astype(F32)
            a = jnp.concatenate([a, jnp.zeros((rank, LANES - rank), F32)], axis=1)
            first = (i * take + j) * rank
            share_ref[first : first + rank, :] = a.astype(BF)

    sends = [pltpu.make_async_copy(share_ref, share_out, out_sems.at[local])]
    sends[0].start()
    for lp in range(local):
        panel_copies[lp].wait()
        keep = lax.broadcasted_iota(jnp.int32, (rank, LANES), 0) < ranks[lp]
        for k in range(n_pair):
            for w in range(wide):
                start = pl.multiple_of(((me ^ k) * wide + w) * LANES, LANES)
                x = panels[lp, :, pl.ds(start, LANES)].astype(F32)
                chunks[me ^ k, lp, w * rank : (w + 1) * rank, :] = jnp.where(keep, x, 0.0).astype(BF)
        if rest:
            for t in range(n_pair * rest // LANES):
                start = n_pair * wide * LANES + t * LANES
                x = panels[lp, :, start : start + LANES].astype(F32)
                x = jnp.where(keep, x, 0.0)
                x = jnp.concatenate([x, jnp.zeros((LANES - rank, LANES), F32)], axis=0)
                turned[lp, t * LANES : (t + 1) * LANES, :] = x.T.astype(BF)
            for k in range(n_pair):
                start = pl.multiple_of((me ^ k) * rest, 16)
                chunks[me ^ k, lp, wide * rank :, :] = turned[lp, pl.ds(start, rest), :]
        send = pltpu.make_async_copy(chunks.at[:, lp], chunks_out.at[:, lp], out_sems.at[lp])
        send.start()
        sends.append(send)
    for send in sends:
        send.wait()


def couple_kernel(n_pair, blocks, sides, shape, table, panels, *refs):
    half = n_pair // 2
    mats = refs[: half * sides]
    out_ref, proj, mixed, mat, mix_ref = refs[half * sides :]
    local, rank, part, freqs = shape
    total = n_pair * local
    wide = part // LANES
    rest = part - wide * LANES
    rows = rank // blocks
    lanes = freqs * LANES
    me, aux = lax.axis_index("pair"), lax.axis_index("aux")
    take = freqs // sides

    def keep(first, index, value):
        count = value.shape[0] // GROUP
        proj[first // GROUP : first // GROUP + count, index] = value.astype(BF).reshape(
            count, GROUP, lanes
        )

    half_group = GROUP // 2
    lane = lax.broadcasted_iota(jnp.int32, (half_group, total * GROUP), 1)
    row = lax.broadcasted_iota(jnp.int32, (half_group, total * GROUP), 0)
    column = lane % GROUP
    group = lane // GROUP
    group = (((group // local) ^ me) * local + group % local).astype(F32)
    slots = table.shape[2] // local

    for k in range(n_pair):
        for lp in range(local):
            index = k * local + lp
            acc = jnp.zeros((half_group, total * GROUP), F32)
            for j in range(lp * slots, (lp + 1) * slots):
                acc = acc + jnp.where(group == table[k, 0, j], table[k, 1, j], 0.0)
            both = [
                jnp.where(column == row + shift, acc, 0.0) for shift in (0, half_group)
            ]
            mix_ref[index * GROUP : (index + 1) * GROUP, :] = jnp.concatenate(both, axis=0).astype(
                BF
            )
            for s in range(freqs):
                slot, inner = s // take, s % take
                first = (lp * take + inner) * rank
                piece = mats[slot * half + k % half].at[k // half]
                mat[index, :, s * LANES : (s + 1) * LANES] = piece[first : first + rank, :]
            for w in range(wide):
                found = lax.dot_general(
                    panels[me ^ k, lp, w * rank : (w + 1) * rank, :],
                    mat[index],
                    (((0,), (0,)), ((), ())),
                    preferred_element_type=F32,
                )
                keep(w * LANES, index, found)
            if rest:
                found = jnp.dot(
                    panels[me ^ k, lp, wide * rank :, :][:, :rank],
                    mat[index],
                    preferred_element_type=F32,
                )
                keep(wide * LANES, index, found)

    for g in range(part // GROUP):
        found = jnp.dot(
            mix_ref[...], proj[g].reshape(total * GROUP, lanes), preferred_element_type=F32
        )
        mixed[:, g * GROUP : (g + 1) * GROUP, :] = found.astype(BF).reshape(total, GROUP, lanes)

    for k in range(n_pair):
        parts = []
        for lp in range(local):
            index = k * local + lp
            got = None
            if wide:
                x = jnp.concatenate(
                    [panels[me ^ k, lp, w * rank : (w + 1) * rank, :] for w in range(wide)], axis=1
                )
                got = jnp.dot(x, mixed[index, : wide * LANES, :], preferred_element_type=F32)
            if rest:
                more = lax.dot_general(
                    panels[me ^ k, lp, wide * rank :, :],
                    mixed[index, wide * LANES :, :],
                    (((0,), (0,)), ((), ())),
                    preferred_element_type=F32,
                )[:rank]
                got = more if got is None else got + more
            parts.append(got)
        for h in range(blocks):
            side = aux % 2 ^ (h % 2) if blocks > 1 else 0
            pieces = []
            for lp in range(local):
                for f in range(freqs):
                    here = f * LANES
                    there = ((f // take ^ 1) * take + f % take) * LANES if sides == 2 else here
                    block = parts[lp][h * rows : (h + 1) * rows]
                    value = block[:, here : here + LANES]
                    if sides == 2:
                        value = jnp.where(aux % 2 == 0, value, block[:, there : there + LANES])
                    pieces.append(value)
            out_ref[side, me ^ k, h // 2] = jnp.concatenate(pieces, axis=0).astype(out_ref.dtype)


def body(sizes, panels, amplitudes, drive, pno_energy, occ_energy, frequency, pair_lmo,
         neighbours, pno_ranks, fock_off):
    n_pair, n_aux = sizes
    local, rank, width = panels.shape
    freqs = amplitudes.shape[1]
    total = pair_lmo.shape[0]
    slots = neighbours.shape[1]
    even = rank % n_aux == 0 and n_aux % 2 == 0
    blocks = n_aux if even else 1
    rows = rank // blocks
    part = width // n_pair
    me_pair = lax.axis_index("pair")
    me_aux = lax.axis_index("aux")
    wide = part // LANES
    rest = part - wide * LANES
    chunk_rows = wide * rank + rest
    sides = 2 if n_aux % 2 == 0 and freqs % 2 == 0 else 1
    vmem = pl.BlockSpec(memory_space=pltpu.VMEM)
    smem = pl.BlockSpec(memory_space=pltpu.SMEM)

    share_rows = local * (freqs // sides) * rank + 16
    given = (panels, amplitudes, pair_lmo.T, neighbours, pno_ranks, fock_off)
    spaces = [pltpu.VMEM] * 2 + [pltpu.SMEM] * 4
    outs = pl.pallas_call(
        functools.partial(prep_kernel, n_pair, sides),
        out_shape=[jax.ShapeDtypeStruct((n_pair, local, chunk_rows, LANES), BF)]
        + [jax.ShapeDtypeStruct((share_rows, LANES), BF)],
        in_specs=[pl.BlockSpec(memory_space=pltpu.HBM)] * 6,
        out_specs=[pl.BlockSpec(memory_space=pltpu.HBM)] * 2,
        scratch_shapes=[space(a.shape, a.dtype) for space, a in zip(spaces, given)]
        + [
            pltpu.VMEM((n_pair, local, chunk_rows, LANES), BF),
            pltpu.VMEM((share_rows, LANES), BF),
            pltpu.VMEM((local, max(n_pair * rest, 16), LANES), BF),
            pltpu.SemaphoreType.DMA((5,)),
            pltpu.SemaphoreType.DMA((local,)),
            pltpu.SemaphoreType.DMA((local + 1,)),
        ],
        cost_estimate=pl.CostEstimate(flops=0, bytes_accessed=4 * 2**20, transcendentals=0),
    )(*given)
    chunks, share = outs

    far = n_pair // 2
    other = lax.ppermute(share, "pair", flip(n_pair, far))
    pieces = [jnp.concatenate([share[None], other[None]], axis=0)] + [None] * (far - 1)
    received = lax.all_to_all(chunks, "pair", 0, 0, tiled=True)
    for k in range(1, n_pair):
        if k < far:
            pieces[k] = lax.ppermute(pieces[0], "pair", flip(n_pair, k))
    tail = jnp.stack([piece[:, share_rows - 16 :] for piece in pieces], axis=1)
    table = tail.reshape(n_pair, 16, LANES)[:, :2, : local * slots].astype(F32)
    if sides == 2:
        for k in range(far):
            pieces.append(lax.ppermute(pieces[k], "aux", flip(n_aux, 1)))
    packed = local * freqs * rows
    out_dims = (2 if even else 1, n_pair, max(blocks // 2, 1), packed, LANES)
    flops = 4 * total * part * rank * freqs * LANES
    coupled = pl.pallas_call(
        functools.partial(
            couple_kernel, n_pair, blocks, sides, (local, rank, part, freqs)
        ),
        out_shape=jax.ShapeDtypeStruct(out_dims, BF if even else F32),
        in_specs=[smem] + [vmem] * (1 + far * sides),
        out_specs=vmem,
        scratch_shapes=[
            pltpu.VMEM((part // GROUP, total, GROUP, freqs * LANES), BF),
            pltpu.VMEM((total, part, freqs * LANES), BF),
            pltpu.VMEM((total, rank, freqs * LANES), BF),
            pltpu.VMEM((total * GROUP, total * GROUP), BF),
        ],
        compiler_params=pltpu.CompilerParams(vmem_limit_bytes=40 * 2**20),
        cost_estimate=pl.CostEstimate(flops=flops, bytes_accessed=4 * 2**20, transcendentals=0),
    )(table, received, *pieces)

    if even:
        other = lax.ppermute(coupled[1], "aux", flip(n_aux, 1))
        mine = (coupled[0].astype(F32) + other.astype(F32)).astype(BF)
        mine = mine.reshape((n_pair * (n_aux // 2),) + out_dims[3:])
        groups = [
            [g * n_aux + 2 * h + c for g in range(n_pair) for h in range(n_aux // 2)]
            for c in range(2)
        ]
        parts = lax.all_to_all(
            mine, ("pair", "aux"), 0, 0, axis_index_groups=groups, tiled=True
        )
        coupled_share = jnp.sum(parts.astype(F32), axis=0)[:, :rank].reshape(
            local, freqs, rows * rank
        )
    else:
        flat = coupled.reshape(total, freqs, rank, LANES)[:, :, :, :rank]
        flat = flat.reshape(total, freqs, rank * rank)
        share_aux = lax.psum_scatter(flat, "aux", scatter_dimension=2, tiled=True)
        coupled_share = lax.psum_scatter(share_aux, "pair", scatter_dimension=0, tiled=True)

    share_width = drive.shape[2]
    start = me_aux * share_width
    lmo_ids = jnp.arange(occ_energy.shape[0], dtype=jnp.int32)
    own_lmo = lax.dynamic_slice_in_dim(pair_lmo, me_pair * local, local, 0)
    own_table = (own_lmo[:, :, None] == lmo_ids[None, None, :]).astype(F32)
    occ_pair = jnp.sum(own_table * occ_energy[None, None, :], axis=(1, 2))
    signs = jnp.array([1.0, -1.0], F32)
    if even:
        energy_rows = lax.dynamic_slice_in_dim(pno_energy, me_aux * rows, rows, 1)
        shift = energy_rows[:, :, None] + pno_energy[:, None, :] - occ_pair[:, None, None]
        factor = shift[:, None] - signs[None, :, None, None] * frequency[0]
        amp_rows_own = lax.dynamic_slice_in_dim(amplitudes, me_aux * rows, rows, 2)
        diagonal = (factor * amp_rows_own.astype(F32)).reshape(local, freqs, share_width)
    else:
        shift = pno_energy[:, :, None] + pno_energy[:, None, :] - occ_pair[:, None, None]
        factor = shift[:, None] - signs[None, :, None, None] * frequency[0]
        diagonal = (factor * amplitudes.astype(F32)).reshape(local, freqs, rank * rank)
        diagonal = lax.dynamic_slice_in_dim(diagonal, start, share_width, 2)
    return drive + diagonal + coupled_share


def solution(mesh):
    placed = (
        P("pair", None, "aux"),
        P("pair", None, None, None),
        P("pair", None, "aux"),
        P("pair", None),
        P(),
        P(),
        P(),
        P("pair", None),
        P("pair"),
        P(),
    )
    sizes = (mesh.shape["pair"], mesh.shape["aux"])

    def layer(*args):
        return body(sizes, *args)

    return jax.shard_map(
        layer,
        mesh=mesh,
        in_specs=placed,
        out_specs=P("pair", None, "aux"),
        check_vma=False,
    )
```

```python
import functools

import jax
import jax.numpy as jnp
from jax import lax
from jax.experimental import pallas as pl
from jax.experimental.pallas import tpu as pltpu
from jax.sharding import PartitionSpec as P


LANES = 128
GROUP = 16
BF = jnp.bfloat16
F32 = jnp.float32


def flip(count, bits):
    return [(i, i ^ bits) for i in range(count)]


def prep_kernel(n_pair, sides, *refs):
    inputs, chunks_out, share_out = refs[:6], refs[6], refs[7]
    buffers, (chunks, share_ref, turned, sems, panel_sems, out_sems) = refs[8:14], refs[14:]
    panels, amps, lmo, near, ranks, fock = buffers
    copies = [
        pltpu.make_async_copy(src, dst, sems.at[i])
        for i, (src, dst) in enumerate(zip(inputs[1:], buffers[1:]))
    ]
    panel_copies = [
        pltpu.make_async_copy(inputs[0].at[lp], panels.at[lp], panel_sems.at[lp])
        for lp in range(panels.shape[0])
    ]
    for copy in copies + panel_copies:
        copy.start()
    local, rank, width = panels.shape
    part = width // n_pair
    wide = part // LANES
    rest = part - wide * LANES
    me = lax.axis_index("pair")
    aux = lax.axis_index("aux")
    slots = near.shape[1]
    for copy in copies[1:]:
        copy.wait()

    share_rows = share_ref.shape[0]
    row = lax.broadcasted_iota(jnp.int32, (16, LANES), 0)
    lane = lax.broadcasted_iota(jnp.int32, (16, LANES), 1)
    tail = jnp.zeros((16, LANES), F32)
    for lp in range(local):
        left, right = lmo[0, me * local + lp], lmo[1, me * local + lp]
        ids = [near[lp, k] for k in range(slots)]
        values = [fock[left, lmo[0, i]] + fock[right, lmo[1, i]] for i in ids]
        for k in range(slots):
            total = jnp.float32(0.0)
            fresh = jnp.float32(1.0)
            for j in range(slots):
                same = (ids[j] == ids[k]).astype(F32) if j != k else jnp.float32(1.0)
                total = total + same * values[j]
                if j < k:
                    fresh = fresh * (1.0 - same)
            here = lane == lp * slots + k
            tail = jnp.where(here & (row == 0), ids[k].astype(F32), tail)
            tail = jnp.where(here & (row == 1), total * fresh, tail)
    share_ref[share_rows - 16 :, :] = tail.astype(BF)

    freqs = amps.shape[1]
    take = freqs // sides
    s_first = aux % 2 if sides == 2 else 0
    copies[0].wait()
    for i in range(local):
        for j in range(take):
            a = amps[i, s_first * take + j].astype(F32)
            a = jnp.concatenate([a, jnp.zeros((rank, LANES - rank), F32)], axis=1)
            first = (i * take + j) * rank
            share_ref[first : first + rank, :] = a.astype(BF)

    sends = [pltpu.make_async_copy(share_ref, share_out, out_sems.at[local])]
    sends[0].start()
    for lp in range(local):
        panel_copies[lp].wait()
        keep = lax.broadcasted_iota(jnp.int32, (rank, LANES), 0) < ranks[lp]
        kept = jnp.where(keep, 1.0, 0.0).astype(BF)
        for k in range(n_pair):
            for w in range(wide):
                start = pl.multiple_of(((me ^ k) * wide + w) * LANES, LANES)
                x = panels[lp, :, pl.ds(start, LANES)]
                chunks[me ^ k, lp, w * rank : (w + 1) * rank, :] = x * kept
        if rest:
            for t in range(n_pair * rest // LANES):
                start = n_pair * wide * LANES + t * LANES
                x = panels[lp, :, start : start + LANES].astype(F32)
                x = jnp.where(keep, x, 0.0)
                x = jnp.concatenate([x, jnp.zeros((LANES - rank, LANES), F32)], axis=0)
                turned[lp, t * LANES : (t + 1) * LANES, :] = x.T.astype(BF)
            for k in range(n_pair):
                start = pl.multiple_of((me ^ k) * rest, 16)
                chunks[me ^ k, lp, wide * rank :, :] = turned[lp, pl.ds(start, rest), :]
        send = pltpu.make_async_copy(chunks.at[:, lp], chunks_out.at[:, lp], out_sems.at[lp])
        send.start()
        sends.append(send)
    for send in sends:
        send.wait()


def couple_kernel(n_pair, blocks, sides, shape, table, panels, *refs):
    half = n_pair // 2
    mats = refs[: half * sides]
    out_ref, proj, mixed, mat, mix_ref = refs[half * sides :]
    local, rank, part, freqs = shape
    total = n_pair * local
    wide = part // LANES
    rest = part - wide * LANES
    rows = rank // blocks
    lanes = freqs * LANES
    me, aux = lax.axis_index("pair"), lax.axis_index("aux")
    take = freqs // sides

    def keep(first, index, value):
        count = value.shape[0] // GROUP
        proj[first // GROUP : first // GROUP + count, index] = value.astype(BF).reshape(
            count, GROUP, lanes
        )

    half_group = GROUP // 2
    lane = lax.broadcasted_iota(jnp.int32, (half_group, total * GROUP), 1)
    row = lax.broadcasted_iota(jnp.int32, (half_group, total * GROUP), 0)
    column = lane % GROUP
    group = lane // GROUP
    group = (((group // local) ^ me) * local + group % local).astype(F32)
    slots = table.shape[2] // local

    for k in range(n_pair):
        for lp in range(local):
            index = k * local + lp
            acc = jnp.zeros((half_group, total * GROUP), F32)
            for j in range(lp * slots, (lp + 1) * slots):
                acc = acc + jnp.where(group == table[k, 0, j], table[k, 1, j], 0.0)
            both = [
                jnp.where(column == row + shift, acc, 0.0) for shift in (0, half_group)
            ]
            mix_ref[index * GROUP : (index + 1) * GROUP, :] = jnp.concatenate(both, axis=0).astype(
                BF
            )
            for s in range(freqs):
                slot, inner = s // take, s % take
                first = (lp * take + inner) * rank
                piece = mats[slot * half + k % half].at[k // half]
                mat[index, :, s * LANES : (s + 1) * LANES] = piece[first : first + rank, :]
            for w in range(wide):
                found = lax.dot_general(
                    panels[me ^ k, lp, w * rank : (w + 1) * rank, :],
                    mat[index],
                    (((0,), (0,)), ((), ())),
                    preferred_element_type=F32,
                )
                keep(w * LANES, index, found)
            if rest:
                found = jnp.dot(
                    panels[me ^ k, lp, wide * rank :, :][:, :rank],
                    mat[index],
                    preferred_element_type=F32,
                )
                keep(wide * LANES, index, found)

    for g in range(part // GROUP):
        found = jnp.dot(
            mix_ref[...], proj[g].reshape(total * GROUP, lanes), preferred_element_type=F32
        )
        mixed[:, g * GROUP : (g + 1) * GROUP, :] = found.astype(BF).reshape(total, GROUP, lanes)

    for k in range(n_pair):
        parts = []
        for lp in range(local):
            index = k * local + lp
            got = None
            if wide:
                x = jnp.concatenate(
                    [panels[me ^ k, lp, w * rank : (w + 1) * rank, :] for w in range(wide)], axis=1
                )
                got = jnp.dot(x, mixed[index, : wide * LANES, :], preferred_element_type=F32)
            if rest:
                more = lax.dot_general(
                    panels[me ^ k, lp, wide * rank :, :],
                    mixed[index, wide * LANES :, :],
                    (((0,), (0,)), ((), ())),
                    preferred_element_type=F32,
                )[:rank]
                got = more if got is None else got + more
            parts.append(got)
        for h in range(blocks):
            side = aux % 2 ^ (h % 2) if blocks > 1 else 0
            pieces = []
            for lp in range(local):
                for f in range(freqs):
                    here = f * LANES
                    there = ((f // take ^ 1) * take + f % take) * LANES if sides == 2 else here
                    block = parts[lp][h * rows : (h + 1) * rows]
                    value = block[:, here : here + LANES]
                    if sides == 2:
                        value = jnp.where(aux % 2 == 0, value, block[:, there : there + LANES])
                    pieces.append(value)
            out_ref[side, me ^ k, h // 2] = jnp.concatenate(pieces, axis=0).astype(out_ref.dtype)


def body(sizes, panels, amplitudes, drive, pno_energy, occ_energy, frequency, pair_lmo,
         neighbours, pno_ranks, fock_off):
    n_pair, n_aux = sizes
    local, rank, width = panels.shape
    freqs = amplitudes.shape[1]
    total = pair_lmo.shape[0]
    slots = neighbours.shape[1]
    even = rank % n_aux == 0 and n_aux % 2 == 0
    blocks = n_aux if even else 1
    rows = rank // blocks
    part = width // n_pair
    me_pair = lax.axis_index("pair")
    me_aux = lax.axis_index("aux")
    wide = part // LANES
    rest = part - wide * LANES
    chunk_rows = wide * rank + rest
    sides = 2 if n_aux % 2 == 0 and freqs % 2 == 0 else 1
    vmem = pl.BlockSpec(memory_space=pltpu.VMEM)
    smem = pl.BlockSpec(memory_space=pltpu.SMEM)

    share_rows = local * (freqs // sides) * rank + 16
    given = (panels, amplitudes, pair_lmo.T, neighbours, pno_ranks, fock_off)
    spaces = [pltpu.VMEM] * 2 + [pltpu.SMEM] * 4
    outs = pl.pallas_call(
        functools.partial(prep_kernel, n_pair, sides),
        out_shape=[jax.ShapeDtypeStruct((n_pair, local, chunk_rows, LANES), BF)]
        + [jax.ShapeDtypeStruct((share_rows, LANES), BF)],
        in_specs=[pl.BlockSpec(memory_space=pltpu.HBM)] * 6,
        out_specs=[pl.BlockSpec(memory_space=pltpu.HBM)] * 2,
        scratch_shapes=[space(a.shape, a.dtype) for space, a in zip(spaces, given)]
        + [
            pltpu.VMEM((n_pair, local, chunk_rows, LANES), BF),
            pltpu.VMEM((share_rows, LANES), BF),
            pltpu.VMEM((local, max(n_pair * rest, 16), LANES), BF),
            pltpu.SemaphoreType.DMA((5,)),
            pltpu.SemaphoreType.DMA((local,)),
            pltpu.SemaphoreType.DMA((local + 1,)),
        ],
        cost_estimate=pl.CostEstimate(flops=0, bytes_accessed=4 * 2**20, transcendentals=0),
    )(*given)
    chunks, share = outs

    far = n_pair // 2
    other = lax.ppermute(share, "pair", flip(n_pair, far))
    pieces = [jnp.concatenate([share[None], other[None]], axis=0)] + [None] * (far - 1)
    received = lax.all_to_all(chunks, "pair", 0, 0, tiled=True)
    for k in range(1, n_pair):
        if k < far:
            pieces[k] = lax.ppermute(pieces[0], "pair", flip(n_pair, k))
    tail = jnp.stack([piece[:, share_rows - 16 :] for piece in pieces], axis=1)
    table = tail.reshape(n_pair, 16, LANES)[:, :2, : local * slots].astype(F32)
    if sides == 2:
        for k in range(far):
            pieces.append(lax.ppermute(pieces[k], "aux", flip(n_aux, 1)))
    packed = local * freqs * rows
    out_dims = (2 if even else 1, n_pair, max(blocks // 2, 1), packed, LANES)
    flops = 4 * total * part * rank * freqs * LANES
    coupled = pl.pallas_call(
        functools.partial(
            couple_kernel, n_pair, blocks, sides, (local, rank, part, freqs)
        ),
        out_shape=jax.ShapeDtypeStruct(out_dims, BF if even else F32),
        in_specs=[smem] + [vmem] * (1 + far * sides),
        out_specs=vmem,
        scratch_shapes=[
            pltpu.VMEM((part // GROUP, total, GROUP, freqs * LANES), BF),
            pltpu.VMEM((total, part, freqs * LANES), BF),
            pltpu.VMEM((total, rank, freqs * LANES), BF),
            pltpu.VMEM((total * GROUP, total * GROUP), BF),
        ],
        compiler_params=pltpu.CompilerParams(vmem_limit_bytes=40 * 2**20),
        cost_estimate=pl.CostEstimate(flops=flops, bytes_accessed=4 * 2**20, transcendentals=0),
    )(table, received, *pieces)

    if even:
        other = lax.ppermute(coupled[1], "aux", flip(n_aux, 1))
        mine = (coupled[0].astype(F32) + other.astype(F32)).astype(BF)
        mine = mine.reshape((n_pair * (n_aux // 2),) + out_dims[3:])
        groups = [
            [g * n_aux + 2 * h + c for g in range(n_pair) for h in range(n_aux // 2)]
            for c in range(2)
        ]
        parts = lax.all_to_all(
            mine, ("pair", "aux"), 0, 0, axis_index_groups=groups, tiled=True
        )
        coupled_share = jnp.sum(parts.astype(F32), axis=0)[:, :rank].reshape(
            local, freqs, rows * rank
        )
    else:
        flat = coupled.reshape(total, freqs, rank, LANES)[:, :, :, :rank]
        flat = flat.reshape(total, freqs, rank * rank)
        share_aux = lax.psum_scatter(flat, "aux", scatter_dimension=2, tiled=True)
        coupled_share = lax.psum_scatter(share_aux, "pair", scatter_dimension=0, tiled=True)

    share_width = drive.shape[2]
    start = me_aux * share_width
    lmo_ids = jnp.arange(occ_energy.shape[0], dtype=jnp.int32)
    own_lmo = lax.dynamic_slice_in_dim(pair_lmo, me_pair * local, local, 0)
    own_table = (own_lmo[:, :, None] == lmo_ids[None, None, :]).astype(F32)
    occ_pair = jnp.sum(own_table * occ_energy[None, None, :], axis=(1, 2))
    signs = jnp.array([1.0, -1.0], F32)
    if even:
        energy_rows = lax.dynamic_slice_in_dim(pno_energy, me_aux * rows, rows, 1)
        shift = energy_rows[:, :, None] + pno_energy[:, None, :] - occ_pair[:, None, None]
        factor = shift[:, None] - signs[None, :, None, None] * frequency[0]
        amp_rows_own = lax.dynamic_slice_in_dim(amplitudes, me_aux * rows, rows, 2)
        diagonal = (factor * amp_rows_own.astype(F32)).reshape(local, freqs, share_width)
    else:
        shift = pno_energy[:, :, None] + pno_energy[:, None, :] - occ_pair[:, None, None]
        factor = shift[:, None] - signs[None, :, None, None] * frequency[0]
        diagonal = (factor * amplitudes.astype(F32)).reshape(local, freqs, rank * rank)
        diagonal = lax.dynamic_slice_in_dim(diagonal, start, share_width, 2)
    return drive + diagonal + coupled_share


def solution(mesh):
    placed = (
        P("pair", None, "aux"),
        P("pair", None, None, None),
        P("pair", None, "aux"),
        P("pair", None),
        P(),
        P(),
        P(),
        P("pair", None),
        P("pair"),
        P(),
    )
    sizes = (mesh.shape["pair"], mesh.shape["aux"])

    def layer(*args):
        return body(sizes, *args)

    return jax.shard_map(
        layer,
        mesh=mesh,
        in_specs=placed,
        out_specs=P("pair", None, "aux"),
        check_vma=False,
    )
```
